128 devices in a mesh: prow: 4 (over x), pcol: 32 (over z, y, core).
Axes of the slice: x: 4, y: 4, z: 4, core: 2. Of those that a mesh axis runs over, the one named last changes fastest.
Arguments:
- match_tiles: float32 [128, 8, 128, 128], P('pcol', 'prow'), may hold values from 0.05 to 1
- pattern: int32 [128, 8], replicated, may hold values from 0 to 127, as said below
- kept: int32 [128, 8], replicated, may hold values from 0 to 127, as said below
- panel_order: int32 [32], replicated, may hold values from 0 to 31, as said below
Outputs:
- clusters: float32 [128, 8, 128, 128], P('pcol', 'prow')
The draws below stay inside these ranges and needn't reach their ends.
Inputs may be any that keep to these rules, and one draw needn't show every extreme that they name: `pattern`: slots r * 2 to r * 2 + 1 of a tile column name 2 different tile rows of the r-th of the equal row blocks along prow. Tile column j names itself and tile column j + 1 - 2 * (j % 2) in the row block that holds tile row j. Of the tile columns of one panel, the tile columns of any other panel name at most 1 different ones, and exactly 1 for some pairs of panels. `kept`: as for pattern, with the same 1; every named tile is nonzero in the product of the input matrix with itself. `panel_order`: A permutation in which every entry differs from its index by at most one.
All inputs are finite; a program needn't handle non-finite values.
Results may differ from the reference program's by a relative error of at most 0.0003.
Values sent between devices are 32-bit elements; how exact they have to be, the bound alone decides.
No kernel may reach another device: no remote copies, remote signals or barrier semaphores. Data moves between devices by JAX's collectives and lax.ppermute only.
A program may use at most 64 MiB of HBM per device.

```python
import math
import jax
import jax.numpy as jnp
from jax import lax

TB = 128
CP = 4
S = 2
NT = 128
N_PROW = 4
N_PCOL = 32


def build_tables(seed_key):
    panel_band = N_PCOL // N_PROW
    block_span = CP * panel_band
    first_key, second_key, third_key = jax.random.split(jax.random.fold_in(seed_key, 5), 3)
    order_scores = jax.random.randint(first_key, (N_PCOL, N_PROW, panel_band), 0, 1 << 20) * panel_band + jnp.arange(panel_band, dtype=jnp.int32)
    panel_seq = jnp.argsort(order_scores, axis=-1).astype(jnp.int32)
    column_scores = jax.random.randint(second_key, (N_PCOL, N_PROW, panel_band, CP), 0, 1 << 20) * CP + jnp.arange(CP, dtype=jnp.int32)
    column_perm = jnp.argsort(column_scores, axis=-1).astype(jnp.int32)
    slot_ids = jnp.arange(CP * S, dtype=jnp.int32)
    rounds = slot_ids // panel_band
    places = slot_ids % panel_band
    local_panel = panel_seq[:, :, places]
    perm_rows = jnp.take_along_axis(column_perm, local_panel[..., None], axis=2)
    chosen = jnp.take_along_axis(perm_rows, rounds[None, None, :, None], axis=3)[..., 0]
    block_base = (jnp.arange(N_PROW, dtype=jnp.int32) * block_span)[None, :, None]
    row_ids = (block_base + local_panel * CP + chosen).reshape(N_PCOL, N_PROW, CP, S)
    own_block = jnp.arange(N_PCOL, dtype=jnp.int32) // panel_band
    inside_local_block = (jnp.arange(N_PROW, dtype=jnp.int32)[None, :] == own_block[:, None])[:, :, None, None]
    own_cols = jnp.arange(N_PCOL, dtype=jnp.int32)[:, None] * CP + jnp.arange(CP, dtype=jnp.int32)[None, :]
    partner = own_cols + 1 - 2 * (own_cols % 2)
    pattern_rows = jnp.where(inside_local_block, jnp.stack([own_cols, partner], -1)[:, None], row_ids)
    pair_rows = row_ids.reshape(N_PCOL, N_PROW, CP // 2, 2 * S)
    mix_scores = jax.random.randint(third_key, pair_rows.shape, 0, 1 << 20) * (2 * S) + jnp.arange(2 * S, dtype=jnp.int32)
    mixing = jnp.argsort(mix_scores, axis=-1).astype(jnp.int32)
    mixed = jnp.take_along_axis(pair_rows, mixing, axis=-1).reshape(N_PCOL, N_PROW, CP, S)
    kept_rows = jnp.where(inside_local_block, jnp.stack([partner, own_cols], -1)[:, None], mixed)

    def layout(table):
        return jnp.transpose(table, (0, 2, 1, 3)).reshape(NT, N_PROW * S).astype(jnp.int32)
    return (layout(pattern_rows), layout(kept_rows))


def draw_pattern(key, part):
    return build_tables(key)[0]


def draw_kept(key, part):
    return build_tables(key)[1]


def draw_panel_order(key, part):
    first_key, second_key = jax.random.split(jax.random.fold_in(key, 9))
    offset = jax.random.randint(first_key, (), 0, 2)
    flips = jax.random.randint(second_key, (N_PCOL,), 0, 2)
    index = jnp.arange(N_PCOL, dtype=jnp.int32)
    shifted = index - offset
    pair_low = offset + shifted // 2 * 2
    partner = jnp.where(shifted % 2 == 0, index + 1, index - 1)
    usable = (shifted >= 0) & (partner < N_PCOL) & (partner >= 0)
    chosen = flips[jnp.clip(pair_low, 0, N_PCOL - 1)] == 1
    return jnp.where(usable & chosen, partner, index).astype(jnp.int32)


def block_levels(own_key, dims, pieces, low, top_value):
    factor_of, own = 1.0, jax.random.fold_in(own_key, 6)
    for position, blocks in pieces:
        draws = jnp.exp(jax.random.uniform(jax.random.fold_in(own, position), (blocks,), jnp.float32, low / len(pieces), top_value / len(pieces)))
        factor_of = factor_of * jnp.repeat(draws, dims[position] // blocks).reshape([-1 if axis == position else 1 for axis in range(len(dims))])
    return factor_of


def setup_inputs(seed: int = 0) -> dict:
    keys = jax.random.split(jax.random.key(seed), 5)
    match_tiles = jnp.clip(jnp.exp(math.log(1.0) - 2.9957323 * jax.random.uniform(keys[0], (NT, S * N_PROW, TB, TB), jnp.float32) ** block_levels(keys[0], (NT, S * N_PROW, TB, TB), ((0, 32), (1, 4)), -0.2, 0.2)), 0.05, 1.0)
    pattern = draw_pattern(jax.random.fold_in(keys[4], 71), 0)
    kept = draw_kept(jax.random.fold_in(keys[4], 71), 0)
    panel_order = draw_panel_order(jax.random.fold_in(keys[4], 71), 0)
    return {"match_tiles": match_tiles, "pattern": pattern, "kept": kept, "panel_order": panel_order}


def normalize(match_matrix):
    totals = jnp.sum(match_matrix, axis=(1, 2))
    return match_matrix / totals[:, None, None, :]


def expand(match_matrix, in_pattern, out_pattern):
    def one_column(column_vector):
        rows_here = in_pattern[column_vector]
        strips = match_matrix[rows_here]
        strip_rows = in_pattern[rows_here]
        wanted = out_pattern[column_vector]
        weights = (strip_rows[None, :, :] == wanted[:, None, None]).astype(jnp.float32)
        selected_entries = jnp.einsum("tks,ksab->tkab", weights, strips, precision=lax.Precision.HIGHEST)
        return jnp.einsum("ilzj,lje->ize", selected_entries, match_matrix[column_vector], precision=lax.Precision.HIGHEST)
    return lax.map(one_column, jnp.arange(NT, dtype=jnp.int32))


def reference(match_tiles, pattern, kept, panel_order):
    start_matrix = normalize(match_tiles)
    first_product = expand(start_matrix, pattern, kept)
    initial_iterate_matrix = normalize(first_product * first_product)
    second_product = expand(initial_iterate_matrix, kept, kept)
    second_iterate = normalize(second_product * second_product)
    columns = (panel_order[:, None] * CP + jnp.arange(CP, dtype=jnp.int32)[None, :]).reshape(-1)
    return second_iterate[columns]
```

```python
import functools

import jax
import jax.numpy as jnp
from jax import lax
from jax.experimental import pallas as pl
from jax.experimental.pallas import tpu as pltpu
from jax.sharding import PartitionSpec as P


SMEM = pl.BlockSpec(memory_space=pltpu.SMEM)
VMEM = pl.BlockSpec(memory_space=pltpu.VMEM)
ANY = pl.BlockSpec(memory_space=pl.ANY)


def ring(size, step):
    return [(i, (i + step) % size) for i in range(size)]


def sum_over_rows(partial_value, size):
    total = partial_value
    for step in range(1, size):
        total = total + lax.ppermute(partial_value, "prow", ring(size, step))
    return total


def send_kernel(where_ref, chosen_ref, order_ref, x_ref, total_ref, normal_ref, send_ref, sems):
    panels = send_ref.shape[0]
    band = where_ref[1]
    mine = where_ref[0] // band
    normal_ref[...] = x_ref[...] / total_ref[...][:, None, None, :]

    def copy(slot):
        panel = order_ref[slot]
        piece = pltpu.make_async_copy(
            normal_ref.at[chosen_ref[panel]], send_ref.at[slot], sems.at[slot]
        )
        return panel // band != mine, piece

    @pl.loop(0, panels)
    def _(slot):
        needed, piece = copy(slot)

        @pl.when(needed)
        def _():
            piece.start()

    @pl.loop(0, panels)
    def _(slot):
        needed, piece = copy(slot)

        @pl.when(needed)
        def _():
            piece.wait()


def prepare(where, chosen, order, x, totals):
    cols, share, tile, _ = x.shape
    panels = order.shape[0]
    return pl.pallas_call(
        send_kernel,
        out_shape=(
            jax.ShapeDtypeStruct(x.shape, jnp.float32),
            jax.ShapeDtypeStruct((panels, share, tile, tile), jnp.float32),
        ),
        in_specs=[SMEM, SMEM, SMEM, VMEM, VMEM],
        out_specs=(VMEM, ANY),
        scratch_shapes=[pltpu.SemaphoreType.DMA((panels,))],
        cost_estimate=pl.CostEstimate(flops=x.size, bytes_accessed=5 << 20, transcendentals=0),
    )(where, chosen, order, x, totals)


def split(value):
    high = value.astype(jnp.bfloat16)
    low = (value - high.astype(jnp.float32)).astype(jnp.bfloat16)
    return high, low


def product_kernel(
    permuted, where_ref, order_ref, in_ref, out_pat_ref,
    own_ref, ahead_ref, behind_ref, far_low_ref, far_high_ref, got_ref,
    sq_ref, part_ref, left, acc, sems,
):
    cols, share, tile, _ = own_ref.shape
    panel, row, rows = where_ref[0], where_ref[1], where_ref[2]
    names = rows * share

    def lookup(j, rel, s):
        block = lax.rem(row + rel, rows)
        column = in_ref[(panel * cols + j) * names + block * share + s]
        source = column // cols
        local = source == panel
        place = order_ref[source] if permuted else source
        found = []
        for t in range(share):
            wanted = out_pat_ref[(panel * cols + j) * names + row * share + t]
            hit = wanted < 0
            at = 0
            for u in range(share):
                same = in_ref[column * names + row * share + u] == wanted
                hit = jnp.logical_or(hit, same)
                at = jnp.where(same, u, at)
            target = left.at[j, rel, pl.ds(t * tile, tile), pl.ds(s * tile, tile)]
            sem = sems.at[j, rel, s, t]
            own_copy = pltpu.make_async_copy(own_ref.at[lax.rem(column, cols), at], target, sem)
            got_copy = pltpu.make_async_copy(got_ref.at[place, at], target, sem)
            found.append((hit, local, own_copy, got_copy, t))
        return found

    @pl.loop(0, cols)
    def _(j):
        for rel in range(4):
            for s in range(share):
                for hit, local, own_copy, got_copy, t in lookup(j, rel, s):

                    @pl.when(jnp.logical_and(hit, local))
                    def _():
                        own_copy.start()

                    @pl.when(jnp.logical_and(hit, jnp.logical_not(local)))
                    def _():
                        got_copy.start()

                    @pl.when(jnp.logical_not(hit))
                    def _():
                        left[j, rel, pl.ds(t * tile, tile), pl.ds(s * tile, tile)] = jnp.zeros(
                            (tile, tile), jnp.float32
                        )

    acc[...] = jnp.zeros_like(acc)

    @pl.loop(0, cols)
    def _(j):
        for rel in range(4):
            any_hit = False
            for s in range(share):
                for hit, local, own_copy, got_copy, t in lookup(j, rel, s):
                    any_hit = jnp.logical_or(any_hit, hit)

                    @pl.when(hit)
                    def _():
                        got_copy.wait()

            @pl.when(any_hit)
            def _():
                if rel == 0:
                    right = own_ref[j]
                elif rel == 1:
                    right = ahead_ref[j]
                elif rel == 3:
                    right = behind_ref[j]
                else:
                    half = cols // 2
                    low = far_low_ref[lax.rem(j, half)]
                    high = far_high_ref[lax.rem(j, half)]
                    right = jnp.where(j < half, low, high)
                right_high, right_low = split(right.reshape(share * tile, tile))
                left_high, left_low = split(left[j, rel])
                dot = functools.partial(jnp.dot, preferred_element_type=jnp.float32)
                acc[j] += (
                    dot(left_low, right_high) + dot(left_high, right_low)
                ) + dot(left_high, right_high)

        value = acc[j]
        square = value * value
        sq_ref[j] = square.reshape(share, tile, tile)
        part_ref[pl.ds(j, 1), :] = jnp.sum(square, axis=0, keepdims=True)


def multiply(permuted, where, order, in_pattern, out_pattern, own, gathered, got):
    cols, share, tile, _ = own.shape
    depth = share * tile
    return pl.pallas_call(
        functools.partial(product_kernel, permuted),
        out_shape=(
            jax.ShapeDtypeStruct(own.shape, jnp.float32),
            jax.ShapeDtypeStruct((cols, tile), jnp.float32),
        ),
        in_specs=[SMEM] * 4 + [VMEM] * 5 + [ANY],
        out_specs=(VMEM, VMEM),
        scratch_shapes=[
            pltpu.VMEM((cols, 4, depth, depth), jnp.float32),
            pltpu.VMEM((cols, depth, tile), jnp.float32),
            pltpu.SemaphoreType.DMA((cols, 4, share, share)),
        ],
        cost_estimate=pl.CostEstimate(
            flops=cols * 12 * depth * depth * tile, bytes_accessed=6 << 20, transcendentals=0
        ),
    )(where, order, in_pattern, out_pattern, own, *gathered, got)


def gather_rows(own, size):
    half = own.shape[0] // 2
    behind = lax.ppermute(own, "prow", ring(size, 1))
    ahead = lax.ppermute(own, "prow", ring(size, -1))
    far_low = lax.ppermute(behind[:half], "prow", ring(size, 1))
    far_high = lax.ppermute(ahead[half:], "prow", ring(size, -1))
    return ahead, behind, far_low, far_high


def chosen_columns(pattern, panel, cols):
    per_panel = pattern.reshape(-1, cols * pattern.shape[1])
    return jnp.max(jnp.where(per_panel // cols == panel, per_panel % cols, 0), axis=1)


def local(match_tiles, pattern, kept, panel_order):
    cols = match_tiles.shape[0]
    panels = panel_order.shape[0]
    row = lax.axis_index("prow")
    rows = lax.axis_size("prow")
    place = lax.axis_index("pcol")
    panel = panel_order[place]
    band = panels // rows
    order = panel_order
    flat_pattern = pattern.reshape(-1)
    flat_kept = kept.reshape(-1)

    totals = sum_over_rows(jnp.sum(match_tiles, axis=(1, 2)), rows)
    chosen = chosen_columns(pattern, place, cols)
    normal, send = prepare(jnp.stack([place, band]), chosen, order, match_tiles, totals)
    got = lax.all_to_all(send, "pcol", 0, 0, tiled=True)
    from_below = lax.ppermute(normal, "pcol", [(i, i + 1) for i in range(panels - 1)])
    from_above = lax.ppermute(normal, "pcol", [(i + 1, i) for i in range(panels - 1)])
    own = jnp.where(panel == place, normal, jnp.where(panel < place, from_below, from_above))
    where = jnp.stack([panel, row, jnp.int32(rows)])
    square, part = multiply(
        False, where, order, flat_pattern, flat_kept, own, gather_rows(own, rows), got
    )

    totals = sum_over_rows(part, rows)
    chosen = chosen_columns(kept, panel, cols)
    normal, send = prepare(jnp.stack([panel, band]), chosen, order, square, totals)
    got = lax.all_to_all(send, "pcol", 0, 0, tiled=True)
    square, part = multiply(
        True, where, order, flat_kept, flat_kept, normal, gather_rows(normal, rows), got
    )
    totals = sum_over_rows(part, rows)
    return square / totals[:, None, None, :]


def solution(mesh):
    in_specs = (P("pcol", "prow", None, None), P(), P(), P())
    out_specs = P("pcol", "prow", None, None)
    return jax.shard_map(local, mesh=mesh, in_specs=in_specs, out_specs=out_specs, check_vma=False)
```

```python
import functools

import jax
import jax.numpy as jnp
from jax import lax
from jax.experimental import pallas as pl
from jax.experimental.pallas import tpu as pltpu
from jax.sharding import PartitionSpec as P


SMEM = pl.BlockSpec(memory_space=pltpu.SMEM)
VMEM = pl.BlockSpec(memory_space=pltpu.VMEM)
ANY = pl.BlockSpec(memory_space=pl.ANY)


def ring(size, step):
    return [(i, (i + step) % size) for i in range(size)]


def sum_over_rows(partial_value, size):
    total = partial_value
    for step in range(1, size):
        total = total + lax.ppermute(partial_value, "prow", ring(size, step))
    return total


def send_kernel(where_ref, chosen_ref, order_ref, x_ref, total_ref, send_ref, normal, sems):
    panels = send_ref.shape[0]
    mine, band = where_ref[0], where_ref[1]
    normal[...] = x_ref[...] / total_ref[...][:, None, None, :]

    def each(act):
        @pl.loop(0, panels)
        def _(slot):
            panel = order_ref[slot]

            @pl.when(panel // band != mine // band)
            def _():
                act(
                    pltpu.make_async_copy(
                        normal.at[chosen_ref[panel]], send_ref.at[slot], sems.at[slot]
                    )
                )

    each(lambda piece: piece.start())
    each(lambda piece: piece.wait())


def prepare(where, chosen, order, x, totals):
    cols, share, tile, _ = x.shape
    panels = order.shape[0]
    return pl.pallas_call(
        send_kernel,
        out_shape=jax.ShapeDtypeStruct((panels, share, tile, tile), jnp.float32),
        in_specs=[SMEM, SMEM, SMEM, VMEM, VMEM],
        out_specs=ANY,
        scratch_shapes=[
            pltpu.VMEM(x.shape, jnp.float32),
            pltpu.SemaphoreType.DMA((panels,)),
        ],
        cost_estimate=pl.CostEstimate(flops=x.size, bytes_accessed=5 << 20, transcendentals=0),
    )(where, chosen, order, x, totals)


def split(value):
    high = value.astype(jnp.bfloat16)
    low = (value - high.astype(jnp.float32)).astype(jnp.bfloat16)
    return high, low


def product_kernel(
    permuted, where_ref, order_ref, in_ref, out_pat_ref,
    own_ref, ahead_ref, behind_ref, far_low_ref, far_high_ref, got_ref,
    sq_ref, part_ref, left, totals, sems,
):
    cols, share, tile, _ = own_ref.shape
    panel, row, rows = where_ref[0], where_ref[1], where_ref[2]
    names = rows * share
    half = cols // 2

    def far_of(j):
        return far_low_ref[j] if j < half else far_high_ref[j - half]

    for j in range(cols):
        total = jnp.zeros((1, tile), jnp.float32)
        for piece in (own_ref[j], ahead_ref[j], behind_ref[j], far_of(j)):
            total += jnp.sum(piece.reshape(share * tile, tile), axis=0, keepdims=True)
        totals[pl.ds(j, 1), :] = total

    def named(j, rel, s):
        block = lax.rem(row + rel, rows)
        column = in_ref[(panel * cols + j) * names + block * share + s]
        return column, column // cols == panel

    def found(j, column, t):
        wanted = out_pat_ref[(panel * cols + j) * names + row * share + t]
        hit = wanted < 0
        at = 0
        for u in range(share):
            same = in_ref[column * names + row * share + u] == wanted
            hit = jnp.logical_or(hit, same)
            at = jnp.where(same, u, at)
        return hit, at

    def copy_in(j, rel, s, t, column, at):
        source = column // cols
        place = order_ref[source] if permuted else source
        return pltpu.make_async_copy(
            got_ref.at[place, at],
            left.at[j, rel, pl.ds(t * tile, tile), pl.ds(s * tile, tile)],
            sems.at[j, rel, s, t],
        )

    @pl.loop(0, cols)
    def _(j):
        for rel in range(4):
            for s in range(share):
                column, is_own = named(j, rel, s)
                for t in range(share):
                    hit, at = found(j, column, t)
                    region = (j, rel, pl.ds(t * tile, tile), pl.ds(s * tile, tile))

                    @pl.when(jnp.logical_and(hit, jnp.logical_not(is_own)))
                    def _():
                        copy_in(j, rel, s, t, column, at).start()

                    @pl.when(jnp.logical_and(hit, is_own))
                    def _():
                        local = lax.rem(column, cols)
                        left[region] = own_ref[local, at] / totals[pl.ds(local, 1), :]

                    @pl.when(jnp.logical_not(hit))
                    def _():
                        left[region] = jnp.zeros((tile, tile), jnp.float32)

    for j in range(cols):
        sq_ref[j] = jnp.zeros((share, tile, tile), jnp.float32)
        for rel in range(4):
            any_hit = False
            for s in range(share):
                column, is_own = named(j, rel, s)
                for t in range(share):
                    hit, at = found(j, column, t)
                    any_hit = jnp.logical_or(any_hit, hit)

                    @pl.when(jnp.logical_and(hit, jnp.logical_not(is_own)))
                    def _():
                        copy_in(j, rel, s, t, column, at).wait()

            @pl.when(any_hit)
            def _():
                right = (own_ref[j], ahead_ref[j], far_of(j), behind_ref[j])[rel]
                right_high, right_low = split(right.reshape(share * tile, tile))
                left_high, left_low = split(left[j, rel])
                dot = functools.partial(jnp.dot, preferred_element_type=jnp.float32)
                added = (
                    dot(left_low, right_high) + dot(left_high, right_low)
                ) + dot(left_high, right_high)
                sq_ref[j] += added.reshape(share, tile, tile)

        value = sq_ref[j].reshape(share * tile, tile) / totals[pl.ds(j, 1), :]
        square = value * value
        sq_ref[j] = square.reshape(share, tile, tile)
        part_ref[pl.ds(j, 1), :] = jnp.sum(square, axis=0, keepdims=True)


def multiply(permuted, where, order, in_pattern, out_pattern, own, gathered, got):
    cols, share, tile, _ = own.shape
    depth = share * tile
    return pl.pallas_call(
        functools.partial(product_kernel, permuted),
        out_shape=(
            jax.ShapeDtypeStruct(own.shape, jnp.float32),
            jax.ShapeDtypeStruct((cols, tile), jnp.float32),
        ),
        in_specs=[SMEM] * 4 + [VMEM] * 5 + [ANY],
        out_specs=(VMEM, VMEM),
        scratch_shapes=[
            pltpu.VMEM((cols, 4, depth, depth), jnp.float32),
            pltpu.VMEM((cols, tile), jnp.float32),
            pltpu.SemaphoreType.DMA((cols, 4, share, share)),
        ],
        cost_estimate=pl.CostEstimate(
            flops=cols * 12 * depth * depth * tile, bytes_accessed=6 << 20, transcendentals=0
        ),
    )(where, order, in_pattern, out_pattern, own, *gathered, got)


def gather_rows(own, size):
    half = own.shape[0] // 2
    behind = lax.ppermute(own, "prow", ring(size, 1))
    ahead = lax.ppermute(own, "prow", ring(size, -1))
    far_low = lax.ppermute(behind[:half], "prow", ring(size, 1))
    far_high = lax.ppermute(ahead[half:], "prow", ring(size, -1))
    return ahead, behind, far_low, far_high


def chosen_columns(pattern, panel, cols):
    per_panel = pattern.reshape(-1, cols * pattern.shape[1])
    return jnp.max(jnp.where(per_panel // cols == panel, per_panel % cols, 0), axis=1)


def local(match_tiles, pattern, kept, panel_order):
    cols = match_tiles.shape[0]
    panels = panel_order.shape[0]
    row = lax.axis_index("prow")
    rows = lax.axis_size("prow")
    place = lax.axis_index("pcol")
    panel = panel_order[place]
    band = panels // rows
    order = panel_order
    flat_pattern = pattern.reshape(-1)
    flat_kept = kept.reshape(-1)

    where = jnp.stack([panel, row, jnp.int32(rows)])
    first_where = jnp.stack([place, band])
    second_where = jnp.stack([panel, band])
    first_chosen = chosen_columns(pattern, place, cols)
    second_chosen = chosen_columns(kept, panel, cols)

    totals = sum_over_rows(jnp.sum(match_tiles, axis=(1, 2)), rows)
    from_below = lax.ppermute(match_tiles, "pcol", [(i, i + 1) for i in range(panels - 1)])
    from_above = lax.ppermute(match_tiles, "pcol", [(i + 1, i) for i in range(panels - 1)])
    totals, from_below, from_above = lax.optimization_barrier((totals, from_below, from_above))
    send = prepare(first_where, first_chosen, order, match_tiles, totals)
    got = lax.all_to_all(send, "pcol", 0, 0, tiled=True)
    own = jnp.where(panel == place, match_tiles, jnp.where(panel < place, from_below, from_above))
    square, part = multiply(
        False, where, order, flat_pattern, flat_kept, own, gather_rows(own, rows), got
    )

    totals = sum_over_rows(part, rows)
    send = prepare(second_where, second_chosen, order, square, totals)
    got = lax.all_to_all(send, "pcol", 0, 0, tiled=True)
    square, part = multiply(
        True, where, order, flat_kept, flat_kept, square, gather_rows(square, rows), got
    )
    totals = sum_over_rows(part, rows)
    return square / totals[:, None, None, :]


def solution(mesh):
    in_specs = (P("pcol", "prow", None, None), P(), P(), P())
    out_specs = P("pcol", "prow", None, None)
    return jax.shard_map(local, mesh=mesh, in_specs=in_specs, out_specs=out_specs, check_vma=False)
```

```python
import functools

import jax
import jax.numpy as jnp
from jax import lax
from jax.experimental import pallas as pl
from jax.experimental.pallas import tpu as pltpu
from jax.sharding import PartitionSpec as P


SMEM = pl.BlockSpec(memory_space=pltpu.SMEM)
VMEM = pl.BlockSpec(memory_space=pltpu.VMEM)
ANY = pl.BlockSpec(memory_space=pl.ANY)

LANES = 128
SEND, FIRST, HOP, SECOND, MISFIT = range(5)
TILE_BIT, SENT_BIT = 4, 8


def ring(size, step):
    return [(i, (i + step) % size) for i in range(size)]


def row_sums(partial_value, size):
    return (partial_value,) + tuple(
        lax.ppermute(partial_value, "prow", ring(size, step)) for step in range(1, size)
    )


def plan_kernel(permuted, whole, scal_ref, order_ref, in_ref, out_ref, plan_ref, grid_ref):
    place, row, rows, cols, depth = (scal_ref[i] for i in range(5))
    share = in_ref.shape[0] // 4
    shape = (LANES, LANES)
    down = lax.broadcasted_iota(jnp.int32, shape, 0)
    along = lax.broadcasted_iota(jnp.int32, shape, 1)
    held = jnp.broadcast_to(order_ref[...], shape)
    if permuted:
        diagonal = jnp.where(down == along, held, 0)
        source = jnp.broadcast_to(jnp.sum(diagonal, axis=1, keepdims=True), shape)
    else:
        source = jnp.where(down < depth * 4, down, -1)
    names = in_ref[...]
    panels, inside = names // 4, lax.rem(names, 4)
    groups = (down // 4 == held).astype(jnp.bfloat16)
    level, wide = lax.div(down, depth), lax.div(along, depth)
    same_level = level == wide
    valid = jnp.logical_and(down < depth * 4, along < depth * 4)
    spread = jnp.logical_and(
        jnp.logical_and(lax.rem(down, depth) == lax.rem(along, depth), valid),
        jnp.logical_not(same_level),
    ).astype(jnp.bfloat16)
    other = jnp.logical_and(valid, source != held)

    def product(left, right):
        return jnp.dot(
            left.astype(jnp.bfloat16), right.astype(jnp.bfloat16),
            preferred_element_type=jnp.float32,
        )

    def gathered(block):
        kept = [out_ref[pl.ds(block * share + t, 1), :] for t in range(share)]
        hits = []
        for u in range(share):
            line = jnp.broadcast_to(in_ref[pl.ds(block * share + u, 1), :], names.shape)
            value = jnp.take_along_axis(line, names, axis=1)
            hit = value == kept[0]
            for t in range(1, share):
                hit = jnp.logical_or(hit, value == kept[t])
            hits.append(hit.astype(jnp.float32))
        return hits

    def analyse(block):
        hits = gathered(block)
        zero = jnp.zeros(shape, jnp.float32)
        found, named, column = [zero] * share, zero, zero
        for k in range(names.shape[0]):
            here = (source == panels[k : k + 1, :]).astype(jnp.float32)
            named += here
            column += here * inside[k : k + 1, :].astype(jnp.float32)
            for u in range(share):
                found[u] += here * hits[u][k : k + 1, :]
        found = [jnp.where(other, product(value, groups), 0.0) > 0.5 for value in found]
        named = jnp.maximum(product(named, groups), 1.0)
        column = jnp.floor(product(column, groups) / named + 0.5)
        both = jnp.logical_and(found[0], found[1])
        away = jnp.logical_and(both, jnp.logical_not(same_level)).astype(jnp.float32)
        return found, column, both, away, product(away, spread)

    if whole:
        misfit = jnp.zeros(shape, jnp.float32)
        for block in range(4):
            found, _, both, away, riding = analyse(block)
            need = jnp.logical_or(found[0], found[1])
            crowded = jnp.logical_or(
                riding > 1.5, jnp.logical_and(riding > 0.5, jnp.logical_or(need, both))
            )
            misfit += jnp.where(
                jnp.logical_and(same_level, jnp.logical_or(crowded, both)), 1.0, 0.0
            )
            arriving = product(same_level.astype(jnp.float32), away)
            misfit += jnp.where(jnp.logical_and(valid, arriving > 1.5), 1.0, 0.0)
        total = jnp.sum(jnp.sum(misfit, axis=0, keepdims=True), axis=1, keepdims=True)
        plan_ref[...] = jnp.broadcast_to((total > 0.5).astype(jnp.int32), plan_ref.shape)
        return

    found, column, both, away, riding = analyse(row)
    need = jnp.logical_or(found[0], found[1])
    direct = column + jnp.where(found[0], 0.0, float(TILE_BIT)) + SENT_BIT
    ride = product(away * column, spread) + TILE_BIT + SENT_BIT
    taken = jnp.logical_and(same_level, riding > 0.5)
    code = jnp.where(need, direct, jnp.where(taken, ride, 0.0))
    mine = (lax.broadcasted_iota(jnp.int32, (8, LANES), 1) == place).astype(jnp.float32)
    level_row = (
        lax.div(lax.broadcasted_iota(jnp.int32, (8, LANES), 1), depth) == lax.div(place, depth)
    ).astype(jnp.float32)
    first = lax.dot_general(
        mine.astype(jnp.bfloat16), found[0].astype(jnp.float32).astype(jnp.bfloat16),
        (((1,), (1,)), ((), ())), preferred_element_type=jnp.float32,
    )
    hop = product(level_row, away * (down + 1).astype(jnp.float32))
    grid_ref[0] = code
    grid_ref[1] = jnp.where(both, column + (TILE_BIT + SENT_BIT), 0.0)
    plan_ref[pl.ds(SEND, 1), :] = grid_ref[0, pl.ds(place, 1), :].astype(jnp.int32)
    plan_ref[pl.ds(FIRST, 1), :] = first[:1].astype(jnp.int32)
    plan_ref[pl.ds(HOP, 1), :] = hop[:1].astype(jnp.int32)
    plan_ref[pl.ds(SECOND, 1), :] = grid_ref[1, pl.ds(place, 1), :].astype(jnp.int32)


def plan(permuted, whole, scal, order_line, in_pattern, out_pattern):
    return pl.pallas_call(
        functools.partial(plan_kernel, permuted, whole),
        out_shape=jax.ShapeDtypeStruct((8, LANES), jnp.int32),
        in_specs=[SMEM, VMEM, VMEM, VMEM],
        out_specs=VMEM,
        scratch_shapes=[pltpu.VMEM((2, LANES, LANES), jnp.float32)],
        cost_estimate=pl.CostEstimate(
            flops=(4 if whole else 1) << 23, bytes_accessed=1 << 14, transcendentals=0
        ),
    )(scal, order_line, in_pattern, out_pattern)


def send_kernel(line, plan_ref, x_ref, *rest):
    *sums, send_ref, normal, sems = rest
    panels = send_ref.shape[0]
    total = sums[0][...]
    for part in sums[1:]:
        total += part[...]
    normal[...] = x_ref[...] / total[:, None, None, :]

    def each(act):
        @pl.loop(0, panels)
        def _(slot):
            code = plan_ref[line, slot]

            @pl.when(code >= SENT_BIT)
            def _():
                tile = normal.at[code & 3, (code // TILE_BIT) & 1]
                act(pltpu.make_async_copy(tile, send_ref.at[slot], sems.at[slot]))

    each(lambda piece: piece.start())
    each(lambda piece: piece.wait())


def prepare(line, steps, x, sums, panels):
    tile = x.shape[-1]
    return pl.pallas_call(
        functools.partial(send_kernel, line),
        out_shape=jax.ShapeDtypeStruct((panels, tile, tile), jnp.float32),
        in_specs=[SMEM, VMEM] + [VMEM] * len(sums),
        out_specs=ANY,
        scratch_shapes=[
            pltpu.VMEM(x.shape, jnp.float32),
            pltpu.SemaphoreType.DMA((panels,)),
        ],
        cost_estimate=pl.CostEstimate(flops=x.size, bytes_accessed=3 << 20, transcendentals=0),
    )(steps, x, *sums)


def hop_kernel(scal_ref, plan_ref, got_ref, *rest):
    *outs, sems = rest
    place, depth = scal_ref[0], scal_ref[4]
    pieces = []
    for step, out in enumerate(outs):
        target = lax.rem(place + (step + 1) * depth, 4 * depth)
        slot = jnp.maximum(plan_ref[HOP, target] - 1, 0)
        pieces.append(pltpu.make_async_copy(got_ref.at[slot], out, sems.at[step]))
    for piece in pieces:
        piece.start()
    for piece in pieces:
        piece.wait()


def hop_tiles(scal, steps, got):
    tile = jax.ShapeDtypeStruct(got.shape[1:], jnp.float32)
    return pl.pallas_call(
        hop_kernel,
        out_shape=(tile,) * 3,
        in_specs=[SMEM, SMEM, ANY],
        out_specs=(VMEM,) * 3,
        scratch_shapes=[pltpu.SemaphoreType.DMA((3,))],
        cost_estimate=pl.CostEstimate(flops=0, bytes_accessed=6 << 16, transcendentals=0),
    )(scal, steps, got)


def split(value):
    high = value.astype(jnp.bfloat16)
    low = (value - high.astype(jnp.float32)).astype(jnp.bfloat16)
    return high, low


def product_kernel(
    permuted, scal_ref, order_ref, plan_ref, in_ref, out_pat_ref,
    own_ref, ahead_ref, behind_ref, far_low_ref, far_high_ref, got_ref, *rest,
):
    *extra_refs, sq_ref, part_ref, left, totals, sems = rest
    cols, share, tile, _ = own_ref.shape
    place, row, rows, depth = scal_ref[0], scal_ref[1], scal_ref[2], scal_ref[4]
    panel = order_ref[place]
    half = cols // 2

    def far_of(j):
        return far_low_ref[j] if j < half else far_high_ref[j - half]

    for j in range(cols):
        total = jnp.zeros((1, tile), jnp.float32)
        for piece in (own_ref[j], ahead_ref[j], behind_ref[j], far_of(j)):
            total += jnp.sum(piece.reshape(share * tile, tile), axis=0, keepdims=True)
        totals[pl.ds(j, 1), :] = total

    def named(j, rel, s):
        block = lax.rem(row + rel, rows)
        column = in_ref[block * share + s, panel * cols + j]
        return column, column // cols == panel

    def found(j, column, t):
        wanted = out_pat_ref[row * share + t, panel * cols + j]
        hit = wanted < 0
        at = 0
        for u in range(share):
            same = in_ref[row * share + u, column] == wanted
            hit = jnp.logical_or(hit, same)
            at = jnp.where(same, u, at)
        return hit, at

    def target_of(j, rel, s, t):
        return (
            left.at[j, rel, pl.ds(t * tile, tile), pl.ds(s * tile, tile)],
            sems.at[j, rel, s, t],
        )

    def start(j, rel, s, t, column, at):
        source = column // cols
        origin = order_ref[source] if permuted else source
        extra = jnp.logical_and(at == 1, plan_ref[FIRST, origin] > 0)
        target, sem = target_of(j, rel, s, t)

        @pl.when(jnp.logical_not(extra))
        def _():
            pltpu.make_async_copy(got_ref.at[origin], target, sem).start()

        if len(extra_refs) == 1:

            @pl.when(extra)
            def _():
                pltpu.make_async_copy(extra_refs[0].at[origin], target, sem).start()

        else:
            step = lax.rem(place // depth - origin // depth + 4, 4)
            for distance, ref in enumerate(extra_refs):

                @pl.when(jnp.logical_and(extra, step == distance + 1))
                def _():
                    pltpu.make_async_copy(ref, target, sem).start()

    @pl.loop(0, cols)
    def _(j):
        for rel in range(4):
            for s in range(share):
                column, is_own = named(j, rel, s)
                for t in range(share):
                    hit, at = found(j, column, t)
                    region = (j, rel, pl.ds(t * tile, tile), pl.ds(s * tile, tile))

                    @pl.when(jnp.logical_and(hit, jnp.logical_not(is_own)))
                    def _():
                        start(j, rel, s, t, column, at)

                    @pl.when(jnp.logical_and(hit, is_own))
                    def _():
                        local = lax.rem(column, cols)
                        left[region] = own_ref[local, at] / totals[pl.ds(local, 1), :]

                    @pl.when(jnp.logical_not(hit))
                    def _():
                        left[region] = jnp.zeros((tile, tile), jnp.float32)

    def column(j, far):
        sq_ref[j] = jnp.zeros((share, tile, tile), jnp.float32)
        for rel in range(4):
            any_hit = False
            for s in range(share):
                source, is_own = named(j, rel, s)
                for t in range(share):
                    hit, at = found(j, source, t)
                    any_hit = jnp.logical_or(any_hit, hit)

                    @pl.when(jnp.logical_and(hit, jnp.logical_not(is_own)))
                    def _():
                        target, sem = target_of(j, rel, s, t)
                        pltpu.make_async_copy(got_ref.at[0], target, sem).wait()

            @pl.when(any_hit)
            def _():
                right = (own_ref.at[j], ahead_ref.at[j], far, behind_ref.at[j])[rel][...]
                right_high, right_low = split(right.reshape(share * tile, tile))
                left_high, left_low = split(left[j, rel])
                dot = functools.partial(jnp.dot, preferred_element_type=jnp.float32)
                added = (
                    dot(left_low, right_high) + dot(left_high, right_low)
                ) + dot(left_high, right_high)
                sq_ref[j] += added.reshape(share, tile, tile)

        value = sq_ref[j].reshape(share * tile, tile) / totals[pl.ds(j, 1), :]
        square = value * value
        sq_ref[j] = square.reshape(share, tile, tile)
        part_ref[pl.ds(j, 1), :] = jnp.sum(square, axis=0, keepdims=True)

    @pl.loop(0, half)
    def _(j):
        column(j, far_low_ref.at[j])

    @pl.loop(half, cols)
    def _(j):
        column(j, far_high_ref.at[j - half])


def multiply(permuted, scal, order, steps, in_pattern, out_pattern, own, gathered, got, extra):
    cols, share, tile, _ = own.shape
    depth = share * tile
    place_of_extra = [ANY] if len(extra) == 1 else [VMEM] * len(extra)
    return pl.pallas_call(
        functools.partial(product_kernel, permuted),
        out_shape=(
            jax.ShapeDtypeStruct(own.shape, jnp.float32),
            jax.ShapeDtypeStruct((cols, tile), jnp.float32),
        ),
        in_specs=[SMEM] * 5 + [VMEM] * 5 + [ANY] + place_of_extra,
        out_specs=(VMEM, VMEM),
        scratch_shapes=[
            pltpu.VMEM((cols, 4, depth, depth), jnp.float32),
            pltpu.VMEM((cols, tile), jnp.float32),
            pltpu.SemaphoreType.DMA((cols, 4, share, share)),
        ],
        cost_estimate=pl.CostEstimate(
            flops=cols * 12 * depth * depth * tile, bytes_accessed=6 << 20, transcendentals=0
        ),
    )(scal, order, steps, in_pattern, out_pattern, own, *gathered, got, *extra)


def divide_kernel(x_ref, *rest):
    *sums, out_ref = rest
    total = sums[0][...]
    for part in sums[1:]:
        total += part[...]
    out_ref[...] = x_ref[...] / total[:, None, None, :]


def divided(x, sums):
    return pl.pallas_call(
        divide_kernel,
        out_shape=jax.ShapeDtypeStruct(x.shape, jnp.float32),
        in_specs=[VMEM] * (1 + len(sums)),
        out_specs=VMEM,
        cost_estimate=pl.CostEstimate(flops=x.size, bytes_accessed=1 << 20, transcendentals=0),
    )(x, *sums)


def gather_rows(own, size):
    half = own.shape[0] // 2
    behind = lax.ppermute(own, "prow", ring(size, 1))
    ahead = lax.ppermute(own, "prow", ring(size, -1))
    far_low = lax.ppermute(behind[:half], "prow", ring(size, 1))
    far_high = lax.ppermute(ahead[half:], "prow", ring(size, -1))
    return ahead, behind, far_low, far_high


def expand(permuted, scal, order, steps, misfit, in_pattern, out_pattern, x, sums, own, rows):
    panels = order.shape[0]
    depth = panels // 4
    got = lax.all_to_all(prepare(SEND, steps, x, sums, panels), "pcol", 0, 0, tiled=True)
    gathered = gather_rows(own, rows)
    finish = functools.partial(
        multiply, permuted, scal, order, steps, in_pattern, out_pattern, own, gathered, got
    )

    def by_level(_):
        tiles = hop_tiles(scal, steps, got)
        return finish(
            tuple(
                lax.ppermute(tile, "pcol", ring(panels, (step + 1) * depth))
                for step, tile in enumerate(tiles)
            )
        )

    def by_second(_):
        more = prepare(SECOND, steps, x, sums, panels)
        return finish((lax.all_to_all(more, "pcol", 0, 0, tiled=True),))

    return lax.cond(misfit[0, 0] > 0, by_second, by_level, 0)


def local(match_tiles, pattern, kept, panel_order):
    cols = match_tiles.shape[0]
    panels = panel_order.shape[0]
    row = lax.axis_index("prow")
    rows = lax.axis_size("prow")
    place = lax.axis_index("pcol")
    panel = panel_order[place]
    order = panel_order
    order_line = jnp.pad(order, (0, LANES - panels), constant_values=-2)[None]
    pattern_rows = pattern.T
    kept_rows = kept.T
    scal = jnp.stack(
        [place, row, jnp.int32(rows), jnp.int32(cols), jnp.int32(panels // 4)]
    )
    first_plan = plan(False, False, scal, order_line, pattern_rows, kept_rows)

    sums = row_sums(jnp.sum(match_tiles, axis=(1, 2)), rows)
    from_below = lax.ppermute(match_tiles, "pcol", [(i, i + 1) for i in range(panels - 1)])
    from_above = lax.ppermute(match_tiles, "pcol", [(i + 1, i) for i in range(panels - 1)])
    sums, from_below, from_above = lax.optimization_barrier((sums, from_below, from_above))
    own = jnp.where(panel == place, match_tiles, jnp.where(panel < place, from_below, from_above))
    first_misfit = plan(False, True, scal, order_line, pattern_rows, kept_rows)
    second_plan = plan(True, False, scal, order_line, kept_rows, kept_rows)
    second_misfit = plan(True, True, scal, order_line, kept_rows, kept_rows)
    square, part = expand(
        False, scal, order, first_plan, first_misfit, pattern_rows, kept_rows,
        match_tiles, sums, own, rows,
    )
    sums = row_sums(part, rows)
    square, part = expand(
        True, scal, order, second_plan, second_misfit, kept_rows, kept_rows,
        square, sums, square, rows,
    )
    return divided(square, row_sums(part, rows))


def solution(mesh):
    in_specs = (P("pcol", "prow", None, None), P(), P(), P())
    out_specs = P("pcol", "prow", None, None)
    return jax.shard_map(local, mesh=mesh, in_specs=in_specs, out_specs=out_specs, check_vma=False)
```

```python
import functools

import jax
import jax.numpy as jnp
from jax import lax
from jax.experimental import pallas as pl
from jax.experimental.pallas import tpu as pltpu
from jax.sharding import PartitionSpec as P


SMEM = pl.BlockSpec(memory_space=pltpu.SMEM)
VMEM = pl.BlockSpec(memory_space=pltpu.VMEM)
ANY = pl.BlockSpec(memory_space=pl.ANY)

LANES = 128
SEND, FIRST, HOP, SECOND, _ = range(5)
TILE_BIT, SENT_BIT = 4, 8


def ring(size, step):
    return [(i, (i + step) % size) for i in range(size)]


def row_sums(partial_value, size):
    sums = [partial_value]
    for step in range(1, size):
        sums.append(lax.ppermute(partial_value, "prow", ring(size, step)))
    return tuple(sums)


def plan_kernel(
    permuted, whole, scal_ref, order_ref, in_ref, out_ref, plan_ref, grid_ref, line_ref
):
    place, row, _, _, depth = (scal_ref[i] for i in range(5))
    share = in_ref.shape[0] // 4
    shape = (LANES, LANES)
    down = lax.broadcasted_iota(jnp.int32, shape, 0)
    along = lax.broadcasted_iota(jnp.int32, shape, 1)
    line_ref[...] = jnp.full(line_ref.shape, -2, jnp.int32)
    line_ref[:1, : order_ref.shape[1]] = order_ref[...]
    held = jnp.broadcast_to(line_ref[:1, :], shape)
    if permuted:
        diagonal = jnp.where(down == along, held, 0)
        source = jnp.broadcast_to(jnp.sum(diagonal, axis=1, keepdims=True), shape)
    else:
        source = jnp.where(down < depth * 4, down, -1)
    names = in_ref[...]
    panels, inside = names // 4, lax.rem(names, 4)
    groups = (down // 4 == held).astype(jnp.bfloat16)
    level, wide = lax.div(down, depth), lax.div(along, depth)
    same_level = level == wide
    valid = jnp.logical_and(down < depth * 4, along < depth * 4)
    spread = jnp.logical_and(
        jnp.logical_and(lax.rem(down, depth) == lax.rem(along, depth), valid),
        jnp.logical_not(same_level),
    ).astype(jnp.bfloat16)
    other = jnp.logical_and(valid, source != held)

    def product(left, right):
        return jnp.dot(
            left.astype(jnp.bfloat16), right.astype(jnp.bfloat16),
            preferred_element_type=jnp.float32,
        )

    def gathered(block):
        kept = [out_ref[pl.ds(block * share + t, 1), :] for t in range(share)]
        hits = []
        for u in range(share):
            line = jnp.broadcast_to(in_ref[pl.ds(block * share + u, 1), :], names.shape)
            value = jnp.take_along_axis(line, names, axis=1)
            hit = value == kept[0]
            for t in range(1, share):
                hit = jnp.logical_or(hit, value == kept[t])
            hits.append(hit.astype(jnp.float32))
        return hits

    def analyse(block):
        hits = gathered(block)
        zero = jnp.zeros(shape, jnp.float32)
        found, named, column = [zero] * share, zero, zero
        for k in range(names.shape[0]):
            here = (source == panels[k : k + 1, :]).astype(jnp.float32)
            named += here
            column += here * inside[k : k + 1, :].astype(jnp.float32)
            for u in range(share):
                found[u] += here * hits[u][k : k + 1, :]
        found = [jnp.where(other, product(value, groups), 0.0) > 0.5 for value in found]
        named = jnp.maximum(product(named, groups), 1.0)
        column = jnp.floor(product(column, groups) / named + 0.5)
        both = jnp.logical_and(found[0], found[1])
        away = jnp.logical_and(both, jnp.logical_not(same_level)).astype(jnp.float32)
        return found, column, both, away, product(away, spread)

    if whole:
        misfit = jnp.zeros(shape, jnp.float32)
        for block in range(4):
            found, _, both, away, riding = analyse(block)
            need = jnp.logical_or(found[0], found[1])
            crowded = jnp.logical_or(
                riding > 1.5, jnp.logical_and(riding > 0.5, jnp.logical_or(need, both))
            )
            misfit += jnp.where(
                jnp.logical_and(same_level, jnp.logical_or(crowded, both)), 1.0, 0.0
            )
            arriving = product(same_level.astype(jnp.float32), away)
            misfit += jnp.where(jnp.logical_and(valid, arriving > 1.5), 1.0, 0.0)
        total = jnp.sum(jnp.sum(misfit, axis=0, keepdims=True), axis=1, keepdims=True)
        plan_ref[...] = jnp.broadcast_to((total > 0.5).astype(jnp.int32), plan_ref.shape)
        return

    found, column, both, away, riding = analyse(row)
    need = jnp.logical_or(found[0], found[1])
    direct = column + jnp.where(found[0], 0.0, float(TILE_BIT)) + SENT_BIT
    ride = product(away * column, spread) + TILE_BIT + SENT_BIT
    taken = jnp.logical_and(same_level, riding > 0.5)
    code = jnp.where(need, direct, jnp.where(taken, ride, 0.0))
    mine = (lax.broadcasted_iota(jnp.int32, (8, LANES), 1) == place).astype(jnp.float32)
    level_row = (
        lax.div(lax.broadcasted_iota(jnp.int32, (8, LANES), 1), depth) == lax.div(place, depth)
    ).astype(jnp.float32)
    first = lax.dot_general(
        mine.astype(jnp.bfloat16), found[0].astype(jnp.float32).astype(jnp.bfloat16),
        (((1,), (1,)), ((), ())), preferred_element_type=jnp.float32,
    )
    hop = product(level_row, away * (down + 1).astype(jnp.float32))
    grid_ref[0] = code
    grid_ref[1] = jnp.where(both, column + (TILE_BIT + SENT_BIT), 0.0)
    plan_ref[pl.ds(SEND, 1), :] = grid_ref[0, pl.ds(place, 1), :].astype(jnp.int32)
    plan_ref[pl.ds(FIRST, 1), :] = first[:1].astype(jnp.int32)
    plan_ref[pl.ds(HOP, 1), :] = hop[:1].astype(jnp.int32)
    plan_ref[pl.ds(SECOND, 1), :] = grid_ref[1, pl.ds(place, 1), :].astype(jnp.int32)


def plan(permuted, whole, scal, order_line, in_pattern, out_pattern):
    return pl.pallas_call(
        functools.partial(plan_kernel, permuted, whole),
        out_shape=jax.ShapeDtypeStruct((8, LANES), jnp.int32),
        in_specs=[SMEM, VMEM, VMEM, VMEM],
        out_specs=VMEM,
        scratch_shapes=[
            pltpu.VMEM((2, LANES, LANES), jnp.float32),
            pltpu.VMEM((8, LANES), jnp.int32),
        ],
        cost_estimate=pl.CostEstimate(
            flops=(4 if whole else 1) << 23, bytes_accessed=1 << 14, transcendentals=0
        ),
    )(scal, order_line, in_pattern, out_pattern)


def column_kernel(x_ref, part_ref):
    part_ref[...] = jnp.sum(x_ref[...], axis=(1, 2))


def column_partial(x):
    return pl.pallas_call(
        column_kernel,
        out_shape=jax.ShapeDtypeStruct((x.shape[0], x.shape[-1]), jnp.float32),
        in_specs=[VMEM],
        out_specs=VMEM,
        cost_estimate=pl.CostEstimate(flops=x.size, bytes_accessed=4 * x.size, transcendentals=0),
    )(x)


def send_kernel(line, plan_ref, x_ref, *rest):
    *sums, send_ref, normal, sems = rest
    panels = send_ref.shape[0]
    total = sums[0][...]
    for part in sums[1:]:
        total += part[...]
    normal[...] = x_ref[...] / total[:, None, None, :]

    def each(act):
        @pl.loop(0, panels)
        def _(slot):
            code = plan_ref[line, slot]

            @pl.when(code >= SENT_BIT)
            def _():
                tile = normal.at[code & 3, (code // TILE_BIT) & 1]
                act(pltpu.make_async_copy(tile, send_ref.at[slot], sems.at[slot]))

    each(lambda piece: piece.start())
    each(lambda piece: piece.wait())


def prepare(line, steps, x, sums, panels):
    tile = x.shape[-1]
    return pl.pallas_call(
        functools.partial(send_kernel, line),
        out_shape=jax.ShapeDtypeStruct((panels, tile, tile), jnp.float32),
        in_specs=[SMEM, VMEM] + [VMEM] * len(sums),
        out_specs=ANY,
        scratch_shapes=[
            pltpu.VMEM(x.shape, jnp.float32),
            pltpu.SemaphoreType.DMA((panels,)),
        ],
        cost_estimate=pl.CostEstimate(flops=x.size, bytes_accessed=3 << 20, transcendentals=0),
    )(steps, x, *sums)


def hop_kernel(scal_ref, plan_ref, got_ref, *rest):
    *outs, sems = rest
    place, depth = scal_ref[0], scal_ref[4]
    pieces = []
    for step, out in enumerate(outs):
        target = lax.rem(place + (step + 1) * depth, 4 * depth)
        slot = jnp.maximum(plan_ref[HOP, target] - 1, 0)
        pieces.append(pltpu.make_async_copy(got_ref.at[slot], out, sems.at[step]))
    for piece in pieces:
        piece.start()
    for piece in pieces:
        piece.wait()


def hop_tiles(scal, steps, got):
    tile = jax.ShapeDtypeStruct(got.shape[1:], jnp.float32)
    return pl.pallas_call(
        hop_kernel,
        out_shape=(tile,) * 3,
        in_specs=[SMEM, SMEM, ANY],
        out_specs=(VMEM,) * 3,
        scratch_shapes=[pltpu.SemaphoreType.DMA((3,))],
        cost_estimate=pl.CostEstimate(flops=0, bytes_accessed=6 << 16, transcendentals=0),
    )(scal, steps, got)


def split(value):
    high = value.astype(jnp.bfloat16)
    low = (value - high.astype(jnp.float32)).astype(jnp.bfloat16)
    return high, low


def product_kernel(
    permuted, scal_ref, order_ref, plan_ref, in_ref, out_pat_ref,
    own_ref, ahead_ref, behind_ref, far_low_ref, far_high_ref, got_ref, *rest,
):
    *extra_refs, sq_ref, part_ref, left, totals, sems = rest
    cols, share, tile, _ = own_ref.shape
    place, row, rows, depth = scal_ref[0], scal_ref[1], scal_ref[2], scal_ref[4]
    panel = order_ref[place]
    half = cols // 2

    def far_of(j):
        return far_low_ref[j] if j < half else far_high_ref[j - half]

    for j in range(cols):
        total = jnp.zeros((1, tile), jnp.float32)
        for piece in (own_ref[j], ahead_ref[j], behind_ref[j], far_of(j)):
            total += jnp.sum(piece.reshape(share * tile, tile), axis=0, keepdims=True)
        totals[pl.ds(j, 1), :] = total

    def named(j, rel, s):
        block = lax.rem(row + rel, rows)
        column = in_ref[block * share + s, panel * cols + j]
        return column, column // cols == panel

    def found(j, column, t):
        wanted = out_pat_ref[row * share + t, panel * cols + j]
        hit = wanted < 0
        at = 0
        for u in range(share):
            same = in_ref[row * share + u, column] == wanted
            hit = jnp.logical_or(hit, same)
            at = jnp.where(same, u, at)
        return hit, at

    def target_of(j, rel, s, t):
        return (
            left.at[j, rel, pl.ds(t * tile, tile), pl.ds(s * tile, tile)],
            sems.at[j, rel, s, t],
        )

    def start(j, rel, s, t, column, at):
        source = column // cols
        origin = order_ref[source] if permuted else source
        extra = jnp.logical_and(at == 1, plan_ref[FIRST, origin] > 0)
        target, sem = target_of(j, rel, s, t)

        @pl.when(jnp.logical_not(extra))
        def _():
            pltpu.make_async_copy(got_ref.at[origin], target, sem).start()

        if len(extra_refs) == 1:

            @pl.when(extra)
            def _():
                pltpu.make_async_copy(extra_refs[0].at[origin], target, sem).start()

        else:
            step = lax.rem(place // depth - origin // depth + 4, 4)
            for distance, ref in enumerate(extra_refs):

                @pl.when(jnp.logical_and(extra, step == distance + 1))
                def _():
                    pltpu.make_async_copy(ref, target, sem).start()

    @pl.loop(0, cols)
    def _(j):
        for rel in range(4):
            for s in range(share):
                column, is_own = named(j, rel, s)
                for t in range(share):
                    hit, at = found(j, column, t)
                    region = (j, rel, pl.ds(t * tile, tile), pl.ds(s * tile, tile))

                    @pl.when(jnp.logical_and(hit, jnp.logical_not(is_own)))
                    def _():
                        start(j, rel, s, t, column, at)

                    @pl.when(jnp.logical_and(hit, is_own))
                    def _():
                        local = lax.rem(column, cols)
                        left[region] = own_ref[local, at] / totals[pl.ds(local, 1), :]

                    @pl.when(jnp.logical_not(hit))
                    def _():
                        left[region] = jnp.zeros((tile, tile), jnp.float32)

    def column(j, far):
        sq_ref[j] = jnp.zeros((share, tile, tile), jnp.float32)
        for rel in range(4):
            any_hit = False
            for s in range(share):
                source, is_own = named(j, rel, s)
                for t in range(share):
                    hit, _ = found(j, source, t)
                    any_hit = jnp.logical_or(any_hit, hit)

                    @pl.when(jnp.logical_and(hit, jnp.logical_not(is_own)))
                    def _():
                        target, sem = target_of(j, rel, s, t)
                        pltpu.make_async_copy(got_ref.at[0], target, sem).wait()

            @pl.when(any_hit)
            def _():
                right = (own_ref.at[j], ahead_ref.at[j], far, behind_ref.at[j])[rel][...]
                right_high, right_low = split(right.reshape(share * tile, tile))
                left_high, left_low = split(left[j, rel])
                dot = functools.partial(jnp.dot, preferred_element_type=jnp.float32)
                added = (
                    dot(left_low, right_high) + dot(left_high, right_low)
                ) + dot(left_high, right_high)
                sq_ref[j] += added.reshape(share, tile, tile)

        value = sq_ref[j].reshape(share * tile, tile) / totals[pl.ds(j, 1), :]
        square = value * value
        sq_ref[j] = square.reshape(share, tile, tile)
        part_ref[pl.ds(j, 1), :] = jnp.sum(square, axis=0, keepdims=True)

    @pl.loop(0, half)
    def _(j):
        column(j, far_low_ref.at[j])

    @pl.loop(half, cols)
    def _(j):
        column(j, far_high_ref.at[j - half])


def multiply(permuted, scal, order, steps, in_pattern, out_pattern, own, gathered, got, extra):
    cols, share, tile, _ = own.shape
    depth = share * tile
    place_of_extra = [ANY] if len(extra) == 1 else [VMEM] * len(extra)
    return pl.pallas_call(
        functools.partial(product_kernel, permuted),
        out_shape=(
            jax.ShapeDtypeStruct(own.shape, jnp.float32),
            jax.ShapeDtypeStruct((cols, tile), jnp.float32),
        ),
        in_specs=[SMEM] * 5 + [VMEM] * 5 + [ANY] + place_of_extra,
        out_specs=(VMEM, VMEM),
        scratch_shapes=[
            pltpu.VMEM((cols, 4, depth, depth), jnp.float32),
            pltpu.VMEM((cols, tile), jnp.float32),
            pltpu.SemaphoreType.DMA((cols, 4, share, share)),
        ],
        cost_estimate=pl.CostEstimate(
            flops=cols * 12 * depth * depth * tile, bytes_accessed=6 << 20, transcendentals=0
        ),
    )(scal, order, steps, in_pattern, out_pattern, own, *gathered, got, *extra)


def divide_kernel(x_ref, *rest):
    *sums, out_ref = rest
    total = sums[0][...]
    for part in sums[1:]:
        total += part[...]
    out_ref[...] = x_ref[...] / total[:, None, None, :]


def divided(x, sums):
    return pl.pallas_call(
        divide_kernel,
        out_shape=jax.ShapeDtypeStruct(x.shape, jnp.float32),
        in_specs=[VMEM] * (1 + len(sums)),
        out_specs=VMEM,
        cost_estimate=pl.CostEstimate(flops=x.size, bytes_accessed=1 << 20, transcendentals=0),
    )(x, *sums)


def gather_rows(own, size):
    half = own.shape[0] // 2
    behind = lax.ppermute(own, "prow", ring(size, 1))
    ahead = lax.ppermute(own, "prow", ring(size, -1))
    far_low = lax.ppermute(behind[:half], "prow", ring(size, 1))
    far_high = lax.ppermute(ahead[half:], "prow", ring(size, -1))
    return ahead, behind, far_low, far_high


def expand(permuted, scal, order, steps, misfit, in_pattern, out_pattern, x, sums, own, rows):
    panels = order.shape[0]
    depth = panels // 4
    send = prepare(SEND, steps, x, sums, panels)
    got = lax.all_to_all(send, "pcol", 0, 0, tiled=True)
    gathered = gather_rows(own, rows)
    finish = functools.partial(
        multiply, permuted, scal, order, steps, in_pattern, out_pattern, own, gathered, got
    )

    def by_level(_):
        tiles = hop_tiles(scal, steps, got)
        return finish(
            tuple(
                lax.ppermute(tile, "pcol", ring(panels, (step + 1) * depth))
                for step, tile in enumerate(tiles)
            )
        )

    def by_second(_):
        more = prepare(SECOND, steps, x, sums, panels)
        return finish((lax.all_to_all(more, "pcol", 0, 0, tiled=True),))

    return lax.cond(misfit[0, 0] > 0, by_second, by_level, 0)


def local(match_tiles, pattern, kept, panel_order):
    cols = match_tiles.shape[0]
    panels = panel_order.shape[0]
    row = lax.axis_index("prow")
    rows = lax.axis_size("prow")
    place = lax.axis_index("pcol")
    panel = panel_order[place]
    order = panel_order
    order_line = order[None]
    pattern_rows = pattern.T
    kept_rows = kept.T
    scal = jnp.stack(
        [place, row, jnp.int32(rows), jnp.int32(cols), jnp.int32(panels // 4)]
    )
    first_plan = plan(False, False, scal, order_line, pattern_rows, kept_rows)

    sums = row_sums(column_partial(match_tiles), rows)
    below = [(i, i + 1) for i in range(panels - 1)]
    from_below = lax.ppermute(match_tiles, "pcol", below)
    from_above = lax.ppermute(match_tiles, "pcol", [(j, i) for i, j in below])
    own = jnp.where(panel == place, match_tiles, jnp.where(panel < place, from_below, from_above))
    sums, own = lax.optimization_barrier((sums, own))
    first_misfit = plan(False, True, scal, order_line, pattern_rows, kept_rows)
    second_plan = plan(True, False, scal, order_line, kept_rows, kept_rows)
    second_misfit = plan(True, True, scal, order_line, kept_rows, kept_rows)
    square, part = expand(
        False, scal, order, first_plan, first_misfit, pattern_rows, kept_rows,
        match_tiles, sums, own, rows,
    )
    sums = row_sums(part, rows)
    square, part = expand(
        True, scal, order, second_plan, second_misfit, kept_rows, kept_rows,
        square, sums, square, rows,
    )
    return divided(square, row_sums(part, rows))


def solution(mesh):
    in_specs = (P("pcol", "prow", None, None), P(), P(), P())
    out_specs = P("pcol", "prow", None, None)
    return jax.shard_map(local, mesh=mesh, in_specs=in_specs, out_specs=out_specs, check_vma=False)
```

```python
import functools

import jax
import jax.numpy as jnp
from jax import lax
from jax.experimental import pallas as pl
from jax.experimental.pallas import tpu as pltpu
from jax.sharding import PartitionSpec as P


SMEM = pl.BlockSpec(memory_space=pltpu.SMEM)
VMEM = pl.BlockSpec(memory_space=pltpu.VMEM)
ANY = pl.BlockSpec(memory_space=pl.ANY)

LANES = 128
SEND, FIRST, HOP, SECOND, MISFIT = range(5)
TILE_BIT, SENT_BIT = 4, 8


def ring(size, step):
    return [(i, (i + step) % size) for i in range(size)]


def row_sums(partial_value, size):
    sums = [partial_value]
    for step in range(1, size):
        sums.append(lax.ppermute(partial_value, "prow", ring(size, step)))
    return tuple(sums)


def plan_kernel(
    permuted, steps, whole, scal_ref, order_ref, in_ref, out_ref, plan_ref, grid_ref, line_ref
):
    place, row, _, _, depth = (scal_ref[i] for i in range(5))
    share = in_ref.shape[0] // 4
    shape = (LANES, LANES)
    down = lax.broadcasted_iota(jnp.int32, shape, 0)
    along = lax.broadcasted_iota(jnp.int32, shape, 1)
    line_ref[...] = jnp.full(line_ref.shape, -2, jnp.int32)
    line_ref[:1, : order_ref.shape[1]] = order_ref[...]
    held = jnp.broadcast_to(line_ref[:1, :], shape)
    if permuted:
        diagonal = jnp.where(down == along, held, 0)
        source = jnp.broadcast_to(jnp.sum(diagonal, axis=1, keepdims=True), shape)
    else:
        source = jnp.where(down < depth * 4, down, -1)
    names = in_ref[...]
    panels, inside = names // 4, lax.rem(names, 4)
    groups = (down // 4 == held).astype(jnp.bfloat16)
    level, wide = lax.div(down, depth), lax.div(along, depth)
    same_level = level == wide
    valid = jnp.logical_and(down < depth * 4, along < depth * 4)
    spread = jnp.logical_and(
        jnp.logical_and(lax.rem(down, depth) == lax.rem(along, depth), valid),
        jnp.logical_not(same_level),
    ).astype(jnp.bfloat16)
    other = jnp.logical_and(valid, source != held)

    def product(left, right):
        return jnp.dot(
            left.astype(jnp.bfloat16), right.astype(jnp.bfloat16),
            preferred_element_type=jnp.float32,
        )

    def gathered(block):
        kept = [out_ref[pl.ds(block * share + t, 1), :] for t in range(share)]
        hits = []
        for u in range(share):
            line = jnp.broadcast_to(in_ref[pl.ds(block * share + u, 1), :], names.shape)
            value = jnp.take_along_axis(line, names, axis=1)
            hit = value == kept[0]
            for t in range(1, share):
                hit = jnp.logical_or(hit, value == kept[t])
            hits.append(hit.astype(jnp.float32))
        return hits

    def analyse(block):
        hits = gathered(block)
        zero = jnp.zeros(shape, jnp.float32)
        found, named, column = [zero] * share, zero, zero
        for k in range(names.shape[0]):
            here = (source == panels[k : k + 1, :]).astype(jnp.float32)
            named += here
            column += here * inside[k : k + 1, :].astype(jnp.float32)
            for u in range(share):
                found[u] += here * hits[u][k : k + 1, :]
        found = [jnp.where(other, product(value, groups), 0.0) > 0.5 for value in found]
        named = jnp.maximum(product(named, groups), 1.0)
        column = jnp.floor(product(column, groups) / named + 0.5)
        both = jnp.logical_and(found[0], found[1])
        away = jnp.logical_and(both, jnp.logical_not(same_level)).astype(jnp.float32)
        return found, column, both, away, product(away, spread)

    def fits():
        misfit = jnp.zeros(shape, jnp.float32)
        for block in range(4):
            found, _, both, away, riding = analyse(block)
            need = jnp.logical_or(found[0], found[1])
            crowded = jnp.logical_or(
                riding > 1.5, jnp.logical_and(riding > 0.5, jnp.logical_or(need, both))
            )
            misfit += jnp.where(
                jnp.logical_and(same_level, jnp.logical_or(crowded, both)), 1.0, 0.0
            )
            arriving = product(same_level.astype(jnp.float32), away)
            misfit += jnp.where(jnp.logical_and(valid, arriving > 1.5), 1.0, 0.0)
        total = jnp.sum(jnp.sum(misfit, axis=0, keepdims=True), axis=1, keepdims=True)
        line = jnp.broadcast_to((total > 0.5).astype(jnp.int32), (1, LANES))
        plan_ref[pl.ds(MISFIT, 1), :] = line

    if whole:
        fits()
    if steps is False:
        return

    found, column, both, away, riding = analyse(row)
    need = jnp.logical_or(found[0], found[1])
    direct = column + jnp.where(found[0], 0.0, float(TILE_BIT)) + SENT_BIT
    ride = product(away * column, spread) + TILE_BIT + SENT_BIT
    taken = jnp.logical_and(same_level, riding > 0.5)
    code = jnp.where(need, direct, jnp.where(taken, ride, 0.0))
    mine = (lax.broadcasted_iota(jnp.int32, (8, LANES), 1) == place).astype(jnp.float32)
    level_row = (
        lax.div(lax.broadcasted_iota(jnp.int32, (8, LANES), 1), depth) == lax.div(place, depth)
    ).astype(jnp.float32)
    first = lax.dot_general(
        mine.astype(jnp.bfloat16), found[0].astype(jnp.float32).astype(jnp.bfloat16),
        (((1,), (1,)), ((), ())), preferred_element_type=jnp.float32,
    )
    hop = product(level_row, away * (down + 1).astype(jnp.float32))
    grid_ref[0] = code
    grid_ref[1] = jnp.where(both, column + (TILE_BIT + SENT_BIT), 0.0)
    plan_ref[pl.ds(SEND, 1), :] = grid_ref[0, pl.ds(place, 1), :].astype(jnp.int32)
    plan_ref[pl.ds(FIRST, 1), :] = first[:1].astype(jnp.int32)
    plan_ref[pl.ds(HOP, 1), :] = hop[:1].astype(jnp.int32)
    plan_ref[pl.ds(SECOND, 1), :] = grid_ref[1, pl.ds(place, 1), :].astype(jnp.int32)


def plans_kernel(parts, scal_ref, order_ref, first_ref, second_ref, *rest):
    *plan_refs, grid_ref, line_ref = rest
    for (permuted, steps, whole), plan_ref in zip(parts, plan_refs):
        plan_kernel(
            permuted, steps, whole, scal_ref, order_ref,
            second_ref if permuted else first_ref, second_ref, plan_ref, grid_ref, line_ref,
        )


def plans(parts, scal, order_line, first_rows, second_rows):
    work = sum((1 if steps else 0) + (4 if whole else 0) for _, steps, whole in parts)
    return pl.pallas_call(
        functools.partial(plans_kernel, parts),
        out_shape=(jax.ShapeDtypeStruct((8, LANES), jnp.int32),) * len(parts),
        in_specs=[SMEM, VMEM, VMEM, VMEM],
        out_specs=(VMEM,) * len(parts),
        scratch_shapes=[
            pltpu.VMEM((2, LANES, LANES), jnp.float32),
            pltpu.VMEM((8, LANES), jnp.int32),
        ],
        cost_estimate=pl.CostEstimate(
            flops=work << 23, bytes_accessed=1 << 14, transcendentals=0
        ),
    )(scal, order_line, first_rows, second_rows)


def column_kernel(x_ref, part_ref):
    part_ref[...] = jnp.sum(x_ref[...], axis=(1, 2))


def column_partial(x):
    return pl.pallas_call(
        column_kernel,
        out_shape=jax.ShapeDtypeStruct((x.shape[0], x.shape[-1]), jnp.float32),
        in_specs=[VMEM],
        out_specs=VMEM,
        cost_estimate=pl.CostEstimate(flops=x.size, bytes_accessed=4 * x.size, transcendentals=0),
    )(x)


def send_kernel(line, plan_ref, x_ref, *rest):
    *sums, send_ref, normal, sems = rest
    panels = send_ref.shape[0]
    total = sums[0][...]
    for part in sums[1:]:
        total += part[...]
    normal[...] = x_ref[...] / total[:, None, None, :]

    def each(act):
        @pl.loop(0, panels)
        def _(slot):
            code = plan_ref[line, slot]

            @pl.when(code >= SENT_BIT)
            def _():
                tile = normal.at[code & 3, (code // TILE_BIT) & 1]
                act(pltpu.make_async_copy(tile, send_ref.at[slot], sems.at[slot]))

    each(lambda piece: piece.start())
    each(lambda piece: piece.wait())


def prepare(line, steps, x, sums, panels):
    tile = x.shape[-1]
    return pl.pallas_call(
        functools.partial(send_kernel, line),
        out_shape=jax.ShapeDtypeStruct((panels, tile, tile), jnp.float32),
        in_specs=[SMEM, VMEM] + [VMEM] * len(sums),
        out_specs=ANY,
        scratch_shapes=[
            pltpu.VMEM(x.shape, jnp.float32),
            pltpu.SemaphoreType.DMA((panels,)),
        ],
        cost_estimate=pl.CostEstimate(flops=x.size, bytes_accessed=3 << 20, transcendentals=0),
    )(steps, x, *sums)


def hop_kernel(scal_ref, plan_ref, got_ref, *rest):
    *outs, sems = rest
    place, depth = scal_ref[0], scal_ref[4]
    pieces = []
    for step, out in enumerate(outs):
        target = lax.rem(place + (step + 1) * depth, 4 * depth)
        slot = jnp.maximum(plan_ref[HOP, target] - 1, 0)
        pieces.append(pltpu.make_async_copy(got_ref.at[slot], out, sems.at[step]))
    for piece in pieces:
        piece.start()
    for piece in pieces:
        piece.wait()


def hop_tiles(scal, steps, got):
    tile = jax.ShapeDtypeStruct(got.shape[1:], jnp.float32)
    return pl.pallas_call(
        hop_kernel,
        out_shape=(tile,) * 3,
        in_specs=[SMEM, SMEM, ANY],
        out_specs=(VMEM,) * 3,
        scratch_shapes=[pltpu.SemaphoreType.DMA((3,))],
        cost_estimate=pl.CostEstimate(flops=0, bytes_accessed=6 << 16, transcendentals=0),
    )(scal, steps, got)


def split(value):
    high = value.astype(jnp.bfloat16)
    low = (value - high.astype(jnp.float32)).astype(jnp.bfloat16)
    return high, low


def dot_exactly(left, right):
    left_high, left_low = split(left)
    right_high, right_low = split(right)
    dot = functools.partial(jnp.dot, preferred_element_type=jnp.float32)
    return (dot(left_low, right_high) + dot(left_high, right_low)) + dot(left_high, right_high)


FIRSTS, SECONDS, LIST = 2, 64, 128


def own_kernel(
    permuted, scal_ref, order_ref, plan_ref, in_ref, out_pat_ref,
    own_ref, ahead_ref, behind_ref, far_low_ref, far_high_ref,
    base_ref, totals_ref, right_ref, list_ref,
):
    cols, share, tile, _ = own_ref.shape
    place, row, depth = scal_ref[0], scal_ref[1], scal_ref[4]
    rows = right_ref.shape[1] // share
    panel = order_ref[place]
    home = panel // depth
    half = cols // 2

    for rel in range(4):
        first = lax.rem(row + rel, rows) * share
        for j in range(cols):
            far = far_low_ref.at[j] if j < half else far_high_ref.at[j - half]
            piece = (own_ref.at[j], ahead_ref.at[j], far, behind_ref.at[j])[rel]
            right_ref[j, pl.ds(first, share)] = piece[...]
    for j in range(cols):
        whole = right_ref[j].reshape(rows * share * tile, tile)
        totals_ref[pl.ds(j, 1), :] = jnp.sum(whole, axis=0, keepdims=True)

    def found(j, column, t):
        wanted = out_pat_ref[row * share + t, panel * cols + j]
        hit = wanted < 0
        at = 0
        for u in range(share):
            same = in_ref[row * share + u, column] == wanted
            hit = jnp.logical_or(hit, same)
            at = jnp.where(same, u, at)
        return hit, at

    def remote(place_of, counts):
        j, k = place_of // (rows * share), lax.rem(place_of, rows * share)
        column = in_ref[k, panel * cols + j]
        source = column // cols
        origin = order_ref[source] if permuted else source
        firsts, seconds = counts
        for t in range(share):
            hit, at = found(j, column, t)
            hit = jnp.logical_and(hit, source != panel)
            extra = jnp.logical_and(hit, jnp.logical_and(at == 1, plan_ref[FIRST, origin] > 0))
            simple = jnp.logical_and(hit, jnp.logical_not(extra))
            entry = (place_of * share + t) * 32 + origin

            @pl.when(simple)
            def _():
                list_ref[FIRSTS + firsts] = entry

            @pl.when(extra)
            def _():
                list_ref[SECONDS + seconds] = entry

            firsts = firsts + simple.astype(jnp.int32)
            seconds = seconds + extra.astype(jnp.int32)
        return firsts, seconds

    firsts, seconds = lax.fori_loop(
        0, cols * rows * share, remote, (jnp.int32(0), jnp.int32(0))
    )
    list_ref[0] = firsts
    list_ref[1] = seconds

    @pl.loop(0, cols)
    def _(j):
        base_ref[j] = jnp.zeros((share, tile, tile), jnp.float32)
        for s in range(share):
            k = home * share + s
            column = in_ref[k, panel * cols + j]
            local = lax.rem(column, cols)
            for t in range(share):
                hit, at = found(j, column, t)

                @pl.when(jnp.logical_and(hit, column // cols == panel))
                def _():
                    left = own_ref[local, at] / totals_ref[pl.ds(local, 1), :]
                    base_ref[j, t] += dot_exactly(left, right_ref[j, k])


def own_products(permuted, scal, order, steps, in_pattern, out_pattern, own, gathered):
    cols, share, tile, _ = own.shape
    return pl.pallas_call(
        functools.partial(own_kernel, permuted),
        out_shape=(
            jax.ShapeDtypeStruct(own.shape, jnp.float32),
            jax.ShapeDtypeStruct((cols, tile), jnp.float32),
            jax.ShapeDtypeStruct((cols, 4 * share, tile, tile), jnp.float32),
            jax.ShapeDtypeStruct((LIST,), jnp.int32),
        ),
        in_specs=[SMEM] * 5 + [VMEM] * 5,
        out_specs=(VMEM, VMEM, VMEM, SMEM),
        cost_estimate=pl.CostEstimate(flops=1 << 26, bytes_accessed=5 << 20, transcendentals=0),
    )(scal, order, steps, in_pattern, out_pattern, own, *gathered)


def add_listed(list_ref, number, first, right_ref, acc_ref, fetch, lefts, rights, sems):
    share = acc_ref.shape[1]
    names = right_ref.shape[1]
    count = list_ref[number]

    def where(i):
        entry = list_ref[first + i]
        spot = entry // 32
        column_slot = spot // share
        return (
            column_slot // names, lax.rem(column_slot, names), lax.rem(spot, share),
            lax.rem(entry, 32),
        )

    def right_copy(i, j, k):
        return pltpu.make_async_copy(right_ref.at[j, k], rights.at[i], sems.at[1, i])

    @pl.loop(0, count)
    def _(i):
        j, k, _, origin = where(i)
        right_copy(i, j, k).start()
        fetch(i, origin)

    @pl.loop(0, count)
    def _(i):
        j, k, t, _ = where(i)
        right_copy(i, j, k).wait()
        pltpu.make_async_copy(right_ref.at[j, k], lefts.at[i], sems.at[0, i]).wait()
        acc_ref[j, t] += dot_exactly(lefts[i], rights[i])


def main_kernel(list_ref, base_ref, right_ref, got_ref, acc_ref, lefts, rights, sems):
    acc_ref[...] = base_ref[...]

    def fetch(i, origin):
        pltpu.make_async_copy(got_ref.at[origin], lefts.at[i], sems.at[0, i]).start()

    add_listed(list_ref, 0, FIRSTS, right_ref, acc_ref, fetch, lefts, rights, sems)


def last_kernel(scal_ref, list_ref, acc_in_ref, totals_ref, right_ref, *rest):
    *extra_refs, sq_ref, part_ref, lefts, rights, sems = rest
    cols, share, tile, _ = acc_in_ref.shape
    place, depth = scal_ref[0], scal_ref[4]
    sq_ref[...] = acc_in_ref[...]

    def fetch(i, origin):
        if len(extra_refs) == 1:
            pltpu.make_async_copy(extra_refs[0].at[origin], lefts.at[i], sems.at[0, i]).start()
            return
        step = lax.rem(place // depth - origin // depth + 4, 4)
        for distance, ref in enumerate(extra_refs):

            @pl.when(step == distance + 1)
            def _():
                pltpu.make_async_copy(ref, lefts.at[i], sems.at[0, i]).start()

    add_listed(list_ref, 1, SECONDS, right_ref, sq_ref, fetch, lefts, rights, sems)
    for j in range(cols):
        value = sq_ref[j].reshape(share * tile, tile) / totals_ref[pl.ds(j, 1), :]
        square = value * value
        sq_ref[j] = square.reshape(share, tile, tile)
        part_ref[pl.ds(j, 1), :] = jnp.sum(square, axis=0, keepdims=True)


def list_scratch(right):
    _, _, tile, _ = right.shape
    most = SECONDS - FIRSTS - 2
    return [
        pltpu.VMEM((most, tile, tile), jnp.float32),
        pltpu.VMEM((most, tile, tile), jnp.float32),
        pltpu.SemaphoreType.DMA((2, most)),
    ]


def main_products(tiles, base, right, got):
    return pl.pallas_call(
        main_kernel,
        out_shape=jax.ShapeDtypeStruct(base.shape, jnp.float32),
        in_specs=[SMEM, VMEM, ANY, ANY],
        out_specs=VMEM,
        scratch_shapes=list_scratch(right),
        cost_estimate=pl.CostEstimate(flops=1 << 30, bytes_accessed=3 << 20, transcendentals=0),
    )(tiles, base, right, got)


def last_products(scal, tiles, acc, totals, right, extra):
    cols, _, tile, _ = acc.shape
    return pl.pallas_call(
        last_kernel,
        out_shape=(
            jax.ShapeDtypeStruct(acc.shape, jnp.float32),
            jax.ShapeDtypeStruct((cols, tile), jnp.float32),
        ),
        in_specs=[SMEM, SMEM, VMEM, VMEM, ANY] + [ANY] * len(extra),
        out_specs=(VMEM, VMEM),
        scratch_shapes=list_scratch(right),
        cost_estimate=pl.CostEstimate(flops=1 << 24, bytes_accessed=2 << 20, transcendentals=0),
    )(scal, tiles, acc, totals, right, *extra)


def divide_kernel(x_ref, *rest):
    *sums, out_ref = rest
    total = sums[0][...]
    for part in sums[1:]:
        total += part[...]
    out_ref[...] = x_ref[...] / total[:, None, None, :]


def divided(x, sums):
    return pl.pallas_call(
        divide_kernel,
        out_shape=jax.ShapeDtypeStruct(x.shape, jnp.float32),
        in_specs=[VMEM] * (1 + len(sums)),
        out_specs=VMEM,
        cost_estimate=pl.CostEstimate(flops=x.size, bytes_accessed=1 << 20, transcendentals=0),
    )(x, *sums)


def gather_rows(own, size):
    half = own.shape[0] // 2
    behind = lax.ppermute(own, "prow", ring(size, 1))
    ahead = lax.ppermute(own, "prow", ring(size, -1))
    far_low = lax.ppermute(behind[:half], "prow", ring(size, 1))
    far_high = lax.ppermute(ahead[half:], "prow", ring(size, -1))
    return ahead, behind, far_low, far_high


def expand(permuted, scal, order, steps, misfit, in_pattern, out_pattern, x, sums, own, rows):
    panels = order.shape[0]
    depth = panels // 4
    send = prepare(SEND, steps, x, sums, panels)
    got = lax.all_to_all(send, "pcol", 0, 0, tiled=True)
    gathered = gather_rows(own, rows)
    base, totals, right, tiles = own_products(
        permuted, scal, order, steps, in_pattern, out_pattern, own, gathered
    )

    def by_level(_):
        hops = hop_tiles(scal, steps, got)
        extra = tuple(
            lax.ppermute(tile, "pcol", ring(panels, (step + 1) * depth))
            for step, tile in enumerate(hops)
        )
        acc = main_products(tiles, base, right, got)
        return last_products(scal, tiles, acc, totals, right, extra)

    def by_second(_):
        more = prepare(SECOND, steps, x, sums, panels)
        extra = (lax.all_to_all(more, "pcol", 0, 0, tiled=True),)
        acc = main_products(tiles, base, right, got)
        return last_products(scal, tiles, acc, totals, right, extra)

    return lax.cond(misfit > 0, by_second, by_level, 0)


def local(match_tiles, pattern, kept, panel_order):
    cols = match_tiles.shape[0]
    panels = panel_order.shape[0]
    row = lax.axis_index("prow")
    rows = lax.axis_size("prow")
    place = lax.axis_index("pcol")
    panel = panel_order[place]
    order = panel_order
    order_line = order[None]
    pattern_rows = pattern.T
    kept_rows = kept.T
    scal = jnp.stack(
        [place, row, jnp.int32(rows), jnp.int32(cols), jnp.int32(panels // 4)]
    )
    tables = (scal, order_line, pattern_rows, kept_rows)
    (first_plan,) = plans(((False, True, False),), *tables)

    sums = row_sums(column_partial(match_tiles), rows)
    below = [(i, i + 1) for i in range(panels - 1)]
    from_below = lax.ppermute(match_tiles, "pcol", below)
    from_above = lax.ppermute(match_tiles, "pcol", [(j, i) for i, j in below])
    own = jnp.where(panel == place, match_tiles, jnp.where(panel < place, from_below, from_above))
    sums, own = lax.optimization_barrier((sums, own))
    check, second_plan = plans(((False, False, True), (True, True, True)), *tables)
    first_misfit, second_misfit = check[MISFIT, 0], second_plan[MISFIT, 0]
    square, part = expand(
        False, scal, order, first_plan, first_misfit, pattern_rows, kept_rows,
        match_tiles, sums, own, rows,
    )
    sums = row_sums(part, rows)
    square, part = expand(
        True, scal, order, second_plan, second_misfit, kept_rows, kept_rows,
        square, sums, square, rows,
    )
    return divided(square, row_sums(part, rows))


def solution(mesh):
    in_specs = (P("pcol", "prow", None, None), P(), P(), P())
    out_specs = P("pcol", "prow", None, None)
    return jax.shard_map(local, mesh=mesh, in_specs=in_specs, out_specs=out_specs, check_vma=False)
```

```python
import functools

import jax
import jax.numpy as jnp
from jax import lax
from jax.experimental import pallas as pl
from jax.experimental.pallas import tpu as pltpu
from jax.sharding import PartitionSpec as P


SMEM = pl.BlockSpec(memory_space=pltpu.SMEM)
VMEM = pl.BlockSpec(memory_space=pltpu.VMEM)
ANY = pl.BlockSpec(memory_space=pl.ANY)

LANES = 128
SEND, FIRST, HOP, SECOND, MISFIT = range(5)
TILE_BIT, SENT_BIT = 4, 8


def ring(size, step):
    return [(i, (i + step) % size) for i in range(size)]


def row_sums(partial_value, size):
    sums = [partial_value]
    for step in range(1, size):
        sums.append(lax.ppermute(partial_value, "prow", ring(size, step)))
    return tuple(sums)


def plan_kernel(
    moved, steps, whole, order_ref, in_ref, out_ref, plan_ref, grid_ref, line_ref
):
    place, row = lax.axis_index("pcol"), lax.axis_index("prow")
    panels_all = order_ref.shape[1]
    depth = panels_all // 4
    share = in_ref.shape[0] // 4
    shape = (LANES, LANES)
    down = lax.broadcasted_iota(jnp.int32, shape, 0)
    along = lax.broadcasted_iota(jnp.int32, shape, 1)
    if moved:
        line_ref[...] = jnp.full(line_ref.shape, -2, jnp.int32)
        line_ref[:1, :panels_all] = order_ref[...]
        held = jnp.broadcast_to(line_ref[:1, :], shape)
    else:
        held = jnp.where(along < panels_all, along, -2)
    source = jnp.where(down < panels_all, down, -1)
    names = in_ref[...]
    panels, inside = names // 4, lax.rem(names, 4)
    groups = (down // 4 == held).astype(jnp.bfloat16)
    level, wide = lax.div(down, depth), lax.div(along, depth)
    same_level = level == wide
    valid = jnp.logical_and(down < depth * 4, along < depth * 4)
    spread = jnp.logical_and(
        jnp.logical_and(lax.rem(down, depth) == lax.rem(along, depth), valid),
        jnp.logical_not(same_level),
    ).astype(jnp.bfloat16)
    other = jnp.logical_and(valid, source != held)

    def product(left, right):
        return jnp.dot(
            left.astype(jnp.bfloat16), right.astype(jnp.bfloat16),
            preferred_element_type=jnp.float32,
        )

    def gathered(block):
        kept = [out_ref[pl.ds(block * share + t, 1), :] for t in range(share)]
        hits = []
        for u in range(share):
            line = jnp.broadcast_to(in_ref[pl.ds(block * share + u, 1), :], names.shape)
            value = jnp.take_along_axis(line, names, axis=1)
            hit = value == kept[0]
            for t in range(1, share):
                hit = jnp.logical_or(hit, value == kept[t])
            hits.append(hit.astype(jnp.float32))
        return hits

    def analyse(block):
        hits = gathered(block)
        zero = jnp.zeros(shape, jnp.float32)
        found, named, column = [zero] * share, zero, zero
        for k in range(names.shape[0]):
            here = (source == panels[k : k + 1, :]).astype(jnp.float32)
            named += here
            column += here * inside[k : k + 1, :].astype(jnp.float32)
            for u in range(share):
                found[u] += here * hits[u][k : k + 1, :]
        found = [jnp.where(other, product(value, groups), 0.0) > 0.5 for value in found]
        named = jnp.maximum(product(named, groups), 1.0)
        column = jnp.floor(product(column, groups) / named + 0.5)
        both = jnp.logical_and(found[0], found[1])
        away = jnp.logical_and(both, jnp.logical_not(same_level)).astype(jnp.float32)
        return found, column, both, away, product(away, spread)

    def fits():
        misfit = jnp.zeros(shape, jnp.float32)
        for block in range(4):
            found, _, both, away, riding = analyse(block)
            need = jnp.logical_or(found[0], found[1])
            crowded = jnp.logical_or(
                riding > 1.5, jnp.logical_and(riding > 0.5, jnp.logical_or(need, both))
            )
            misfit += jnp.where(
                jnp.logical_and(same_level, jnp.logical_or(crowded, both)), 1.0, 0.0
            )
            arriving = product(same_level.astype(jnp.float32), away)
            misfit += jnp.where(jnp.logical_and(valid, arriving > 1.5), 1.0, 0.0)
        total = jnp.sum(jnp.sum(misfit, axis=0, keepdims=True), axis=1, keepdims=True)
        line = jnp.broadcast_to((total > 0.5).astype(jnp.int32), (1, LANES))
        plan_ref[pl.ds(MISFIT, 1), :] = line

    if whole:
        fits()
    if steps is False:
        return

    found, column, both, away, riding = analyse(row)
    need = jnp.logical_or(found[0], found[1])
    direct = column + jnp.where(found[0], 0.0, float(TILE_BIT)) + SENT_BIT
    ride = product(away * column, spread) + TILE_BIT + SENT_BIT
    taken = jnp.logical_and(same_level, riding > 0.5)
    code = jnp.where(need, direct, jnp.where(taken, ride, 0.0))
    mine = (lax.broadcasted_iota(jnp.int32, (8, LANES), 1) == place).astype(jnp.float32)
    level_row = (
        lax.div(lax.broadcasted_iota(jnp.int32, (8, LANES), 1), depth) == lax.div(place, depth)
    ).astype(jnp.float32)
    first = lax.dot_general(
        mine.astype(jnp.bfloat16), found[0].astype(jnp.float32).astype(jnp.bfloat16),
        (((1,), (1,)), ((), ())), preferred_element_type=jnp.float32,
    )
    hop = product(level_row, away * (down + 1).astype(jnp.float32))
    grid_ref[0] = code
    grid_ref[1] = jnp.where(both, column + (TILE_BIT + SENT_BIT), 0.0)
    plan_ref[pl.ds(SEND, 1), :] = grid_ref[0, pl.ds(place, 1), :].astype(jnp.int32)
    plan_ref[pl.ds(FIRST, 1), :] = first[:1].astype(jnp.int32)
    plan_ref[pl.ds(HOP, 1), :] = hop[:1].astype(jnp.int32)
    plan_ref[pl.ds(SECOND, 1), :] = grid_ref[1, pl.ds(place, 1), :].astype(jnp.int32)


def plans_kernel(parts, order_ref, first_ref, second_ref, *rest):
    *plan_refs, grid_ref, line_ref = rest
    for (moved, steps, whole), plan_ref in zip(parts, plan_refs):
        in_ref = second_ref if moved else first_ref
        plan_kernel(
            moved, steps, whole, order_ref, in_ref, second_ref, plan_ref, grid_ref, line_ref
        )


def plans(parts, order_line, first_rows, second_rows):
    work = sum((1 if steps else 0) + (4 if whole else 0) for _, steps, whole in parts)
    return pl.pallas_call(
        functools.partial(plans_kernel, parts),
        out_shape=(jax.ShapeDtypeStruct((8, LANES), jnp.int32),) * len(parts),
        in_specs=[VMEM, VMEM, VMEM],
        out_specs=(VMEM,) * len(parts),
        scratch_shapes=[
            pltpu.VMEM((2, LANES, LANES), jnp.float32),
            pltpu.VMEM((8, LANES), jnp.int32),
        ],
        cost_estimate=pl.CostEstimate(
            flops=work << 23, bytes_accessed=1 << 14, transcendentals=0
        ),
    )(order_line, first_rows, second_rows)


def column_kernel(x_ref, part_ref):
    part_ref[...] = jnp.sum(x_ref[...], axis=(1, 2))


def column_partial(x):
    return pl.pallas_call(
        column_kernel,
        out_shape=jax.ShapeDtypeStruct((x.shape[0], x.shape[-1]), jnp.float32),
        in_specs=[VMEM],
        out_specs=VMEM,
        cost_estimate=pl.CostEstimate(flops=x.size, bytes_accessed=4 * x.size, transcendentals=0),
    )(x)


def send_kernel(line, plan_ref, x_ref, *rest):
    *sums, send_ref, normal, sems = rest
    panels = send_ref.shape[0]
    total = sums[0][...]
    for part in sums[1:]:
        total += part[...]
    normal[...] = x_ref[...] / total[:, None, None, :]

    def each(act):
        @pl.loop(0, panels)
        def _(slot):
            code = plan_ref[line, slot]

            @pl.when(code >= SENT_BIT)
            def _():
                tile = normal.at[code & 3, (code // TILE_BIT) & 1]
                act(pltpu.make_async_copy(tile, send_ref.at[slot], sems.at[slot]))

    each(lambda piece: piece.start())
    each(lambda piece: piece.wait())


def prepare(line, steps, x, sums, panels):
    tile = x.shape[-1]
    return pl.pallas_call(
        functools.partial(send_kernel, line),
        out_shape=jax.ShapeDtypeStruct((panels, tile, tile), jnp.float32),
        in_specs=[SMEM, VMEM] + [VMEM] * len(sums),
        out_specs=ANY,
        scratch_shapes=[
            pltpu.VMEM(x.shape, jnp.float32),
            pltpu.SemaphoreType.DMA((panels,)),
        ],
        cost_estimate=pl.CostEstimate(flops=x.size, bytes_accessed=3 << 20, transcendentals=0),
    )(steps, x, *sums)


def hop_kernel(plan_ref, got_ref, *rest):
    *outs, sems = rest
    place = lax.axis_index("pcol")
    depth = got_ref.shape[0] // 4
    pieces = []
    for step, out in enumerate(outs):
        target = lax.rem(place + (step + 1) * depth, 4 * depth)
        slot = jnp.maximum(plan_ref[HOP, target] - 1, 0)
        pieces.append(pltpu.make_async_copy(got_ref.at[slot], out, sems.at[step]))
    for piece in pieces:
        piece.start()
    for piece in pieces:
        piece.wait()


def hop_tiles(steps, got):
    tile = jax.ShapeDtypeStruct(got.shape[1:], jnp.float32)
    return pl.pallas_call(
        hop_kernel,
        out_shape=(tile,) * 3,
        in_specs=[SMEM, ANY],
        out_specs=(VMEM,) * 3,
        scratch_shapes=[pltpu.SemaphoreType.DMA((3,))],
        cost_estimate=pl.CostEstimate(flops=0, bytes_accessed=6 << 16, transcendentals=0),
    )(steps, got)


def split(value):
    high = value.astype(jnp.bfloat16)
    low = (value - high.astype(jnp.float32)).astype(jnp.bfloat16)
    return high, low


def dot_exactly(left, right):
    left_high, left_low = split(left)
    right_high, right_low = split(right)
    dot = functools.partial(jnp.dot, preferred_element_type=jnp.float32)
    return (dot(left_low, right_high) + dot(left_high, right_low)) + dot(left_high, right_high)


FIRSTS, SECONDS, LIST = 2, 64, 128


def matched(in_ref, out_pat_ref, row, share, own_column, column, t):
    wanted = out_pat_ref[row * share + t, own_column]
    hit = wanted < 0
    at = 0
    for u in range(share):
        same = in_ref[row * share + u, column] == wanted
        hit = jnp.logical_or(hit, same)
        at = jnp.where(same, u, at)
    return hit, at


def held_panel(moved, order_ref):
    place = lax.axis_index("pcol")
    return order_ref[place] if moved else place


def list_kernel(moved, cols, share, order_ref, plan_ref, in_ref, out_pat_ref, list_ref):
    row = lax.axis_index("prow")
    panel = held_panel(moved, order_ref)
    names = in_ref.shape[0]

    def remote(place_of, counts):
        own_column = panel * cols + place_of // names
        column = in_ref[lax.rem(place_of, names), own_column]
        origin = column // cols
        firsts, seconds = counts
        for t in range(share):
            hit, at = matched(in_ref, out_pat_ref, row, share, own_column, column, t)
            hit = jnp.logical_and(hit, origin != panel)
            extra = jnp.logical_and(hit, jnp.logical_and(at == 1, plan_ref[FIRST, origin] > 0))
            simple = jnp.logical_and(hit, jnp.logical_not(extra))
            entry = (place_of * share + t) * 32 + origin

            @pl.when(simple)
            def _():
                list_ref[FIRSTS + firsts] = entry

            @pl.when(extra)
            def _():
                list_ref[SECONDS + seconds] = entry

            firsts = firsts + simple.astype(jnp.int32)
            seconds = seconds + extra.astype(jnp.int32)
        return firsts, seconds

    firsts, seconds = lax.fori_loop(0, cols * names, remote, (jnp.int32(0), jnp.int32(0)))
    list_ref[0] = firsts
    list_ref[1] = seconds


def tile_list(moved, cols, share, order, steps, in_pattern, out_pattern):
    return pl.pallas_call(
        functools.partial(list_kernel, moved, cols, share),
        out_shape=jax.ShapeDtypeStruct((LIST,), jnp.int32),
        in_specs=[SMEM] * 4,
        out_specs=SMEM,
        cost_estimate=pl.CostEstimate(flops=1 << 28, bytes_accessed=1 << 14, transcendentals=0),
    )(order, steps, in_pattern, out_pattern)


def own_kernel(
    moved, order_ref, in_ref, out_pat_ref,
    own_ref, ahead_ref, behind_ref, far_low_ref, far_high_ref,
    base_ref, totals_ref, right_ref,
):
    cols, share, tile, _ = own_ref.shape
    row = lax.axis_index("prow")
    rows = right_ref.shape[1] // share
    panel = held_panel(moved, order_ref)
    home = panel // (order_ref.shape[0] // rows)
    half = cols // 2

    for rel in range(4):
        first = lax.rem(row + rel, rows) * share
        for j in range(cols):
            far = far_low_ref.at[j] if j < half else far_high_ref.at[j - half]
            piece = (own_ref.at[j], ahead_ref.at[j], far, behind_ref.at[j])[rel]
            right_ref[j, pl.ds(first, share)] = piece[...]
    for j in range(cols):
        whole = right_ref[j].reshape(rows * share * tile, tile)
        totals_ref[pl.ds(j, 1), :] = jnp.sum(whole, axis=0, keepdims=True)

    @pl.loop(0, cols)
    def _(j):
        base_ref[j] = jnp.zeros((share, tile, tile), jnp.float32)
        for s in range(share):
            k = home * share + s
            own_column = panel * cols + j
            column = in_ref[k, own_column]
            local = lax.rem(column, cols)
            for t in range(share):
                hit, at = matched(in_ref, out_pat_ref, row, share, own_column, column, t)

                @pl.when(jnp.logical_and(hit, column // cols == panel))
                def _():
                    left = own_ref[local, at] / totals_ref[pl.ds(local, 1), :]
                    base_ref[j, t] += dot_exactly(left, right_ref[j, k])


def own_products(moved, order, in_pattern, out_pattern, own, gathered):
    cols, share, tile, _ = own.shape
    return pl.pallas_call(
        functools.partial(own_kernel, moved),
        out_shape=(
            jax.ShapeDtypeStruct(own.shape, jnp.float32),
            jax.ShapeDtypeStruct((cols, tile), jnp.float32),
            jax.ShapeDtypeStruct((cols, 4 * share, tile, tile), jnp.float32),
        ),
        in_specs=[SMEM] * 3 + [VMEM] * 5,
        out_specs=(VMEM, VMEM, VMEM),
        cost_estimate=pl.CostEstimate(flops=1 << 26, bytes_accessed=5 << 20, transcendentals=0),
    )(order, in_pattern, out_pattern, own, *gathered)


def pick_kernel(order_ref, held_ref, below_ref, above_ref, out_ref, sem):
    place = lax.axis_index("pcol")
    panel = order_ref[place]
    for chosen, ref in (
        (panel == place, held_ref), (panel < place, below_ref), (panel > place, above_ref)
    ):

        @pl.when(chosen)
        def _():
            pltpu.make_async_copy(ref, out_ref, sem).start()

    pltpu.make_async_copy(held_ref, out_ref, sem).wait()


def shifted(order, x):
    up = [(i, i + 1) for i in range(order.shape[0] - 1)]
    from_below = lax.ppermute(x, "pcol", up)
    from_above = lax.ppermute(x, "pcol", [(j, i) for i, j in up])
    return pl.pallas_call(
        pick_kernel,
        out_shape=jax.ShapeDtypeStruct(x.shape, jnp.float32),
        in_specs=[SMEM, ANY, ANY, ANY],
        out_specs=VMEM,
        scratch_shapes=[pltpu.SemaphoreType.DMA],
        cost_estimate=pl.CostEstimate(flops=0, bytes_accessed=1 << 20, transcendentals=0),
    )(order, x, from_below, from_above)


def add_listed(list_ref, number, first, right_ref, acc_ref, fetch, lefts, rights, sems):
    share = acc_ref.shape[1]
    names = right_ref.shape[1]
    count = list_ref[number]

    def where(i):
        entry = list_ref[first + i]
        spot = entry // 32
        column_slot = spot // share
        return (
            column_slot // names, lax.rem(column_slot, names), lax.rem(spot, share),
            lax.rem(entry, 32),
        )

    def right_copy(i, j, k):
        return pltpu.make_async_copy(right_ref.at[j, k], rights.at[i], sems.at[1, i])

    @pl.loop(0, count)
    def _(i):
        j, k, _, origin = where(i)
        right_copy(i, j, k).start()
        fetch(i, origin)

    @pl.loop(0, count)
    def _(i):
        j, k, t, _ = where(i)
        right_copy(i, j, k).wait()
        pltpu.make_async_copy(right_ref.at[j, k], lefts.at[i], sems.at[0, i]).wait()
        acc_ref[j, t] += dot_exactly(lefts[i], rights[i])


def main_kernel(list_ref, base_ref, right_ref, got_ref, acc_ref, lefts, rights, sems):
    acc_ref[...] = base_ref[...]

    def fetch(i, origin):
        pltpu.make_async_copy(got_ref.at[origin], lefts.at[i], sems.at[0, i]).start()

    add_listed(list_ref, 0, FIRSTS, right_ref, acc_ref, fetch, lefts, rights, sems)


def last_kernel(depth, list_ref, acc_in_ref, totals_ref, right_ref, *rest):
    *extra_refs, sq_ref, part_ref, lefts, rights, sems = rest
    cols, share, tile, _ = acc_in_ref.shape
    place = lax.axis_index("pcol")
    sq_ref[...] = acc_in_ref[...]

    def fetch(i, origin):
        if len(extra_refs) == 1:
            pltpu.make_async_copy(extra_refs[0].at[origin], lefts.at[i], sems.at[0, i]).start()
            return
        step = lax.rem(place // depth - origin // depth + 4, 4)
        for distance, ref in enumerate(extra_refs):

            @pl.when(step == distance + 1)
            def _():
                pltpu.make_async_copy(ref, lefts.at[i], sems.at[0, i]).start()

    add_listed(list_ref, 1, SECONDS, right_ref, sq_ref, fetch, lefts, rights, sems)
    for j in range(cols):
        value = sq_ref[j].reshape(share * tile, tile) / totals_ref[pl.ds(j, 1), :]
        square = value * value
        sq_ref[j] = square.reshape(share, tile, tile)
        part_ref[pl.ds(j, 1), :] = jnp.sum(square, axis=0, keepdims=True)


def list_scratch(right):
    _, _, tile, _ = right.shape
    most = SECONDS - FIRSTS - 2
    return [
        pltpu.VMEM((most, tile, tile), jnp.float32),
        pltpu.VMEM((most, tile, tile), jnp.float32),
        pltpu.SemaphoreType.DMA((2, most)),
    ]


def main_products(tiles, base, right, got):
    return pl.pallas_call(
        main_kernel,
        out_shape=jax.ShapeDtypeStruct(base.shape, jnp.float32),
        in_specs=[SMEM, VMEM, ANY, ANY],
        out_specs=VMEM,
        scratch_shapes=list_scratch(right),
        cost_estimate=pl.CostEstimate(flops=1 << 30, bytes_accessed=3 << 20, transcendentals=0),
    )(tiles, base, right, got)


def last_products(depth, tiles, acc, totals, right, extra):
    cols, _, tile, _ = acc.shape
    return pl.pallas_call(
        functools.partial(last_kernel, depth),
        out_shape=(
            jax.ShapeDtypeStruct(acc.shape, jnp.float32),
            jax.ShapeDtypeStruct((cols, tile), jnp.float32),
        ),
        in_specs=[SMEM, VMEM, VMEM, ANY] + [ANY] * len(extra),
        out_specs=(VMEM, VMEM),
        scratch_shapes=list_scratch(right),
        cost_estimate=pl.CostEstimate(flops=1 << 24, bytes_accessed=2 << 20, transcendentals=0),
    )(tiles, acc, totals, right, *extra)


def divide_kernel(x_ref, *rest):
    *sums, out_ref = rest
    total = sums[0][...]
    for part in sums[1:]:
        total += part[...]
    out_ref[...] = x_ref[...] / total[:, None, None, :]


def divided(x, sums):
    return pl.pallas_call(
        divide_kernel,
        out_shape=jax.ShapeDtypeStruct(x.shape, jnp.float32),
        in_specs=[VMEM] * (1 + len(sums)),
        out_specs=VMEM,
        cost_estimate=pl.CostEstimate(flops=x.size, bytes_accessed=1 << 20, transcendentals=0),
    )(x, *sums)


def gather_rows(own, size):
    half = own.shape[0] // 2
    behind = lax.ppermute(own, "prow", ring(size, 1))
    ahead = lax.ppermute(own, "prow", ring(size, -1))
    far_low = lax.ppermute(behind[:half], "prow", ring(size, 1))
    far_high = lax.ppermute(ahead[half:], "prow", ring(size, -1))
    return ahead, behind, far_low, far_high


def expand(moved, order, steps, misfit, in_pattern, out_pattern, x, sums, own, rows):
    cols, share = x.shape[:2]
    panels = order.shape[0]
    depth = panels // 4
    send = prepare(SEND, steps, x, sums, panels)
    got = lax.all_to_all(send, "pcol", 0, 0, tiled=True)
    tiles = tile_list(moved, cols, share, order, steps, in_pattern, out_pattern)
    gathered = gather_rows(own, rows)
    base, totals, right = own_products(moved, order, in_pattern, out_pattern, own, gathered)

    def by_level(_):
        hops = hop_tiles(steps, got)
        extra = tuple(
            lax.ppermute(tile, "pcol", ring(panels, (step + 1) * depth))
            for step, tile in enumerate(hops)
        )
        acc = main_products(tiles, base, right, got)
        return last_products(depth, tiles, acc, totals, right, extra)

    def by_second(_):
        more = prepare(SECOND, steps, x, sums, panels)
        extra = (lax.all_to_all(more, "pcol", 0, 0, tiled=True),)
        acc = main_products(tiles, base, right, got)
        return last_products(depth, tiles, acc, totals, right, extra)

    return lax.cond(misfit > 0, by_second, by_level, 0)


def local(match_tiles, pattern, kept, panel_order):
    rows = lax.axis_size("prow")
    order = panel_order
    pattern_rows = pattern.T
    kept_rows = kept.T
    tables = (order[None], pattern_rows, kept_rows)
    (first_plan,) = plans(((False, True, False),), *tables)
    sums = row_sums(column_partial(match_tiles), rows)
    check, second_plan = plans(((False, False, True), (True, True, True)), *tables)
    square, part = expand(
        False, order, first_plan, check[MISFIT, 0], pattern_rows, kept_rows,
        match_tiles, sums, match_tiles, rows,
    )
    sums = row_sums(part, rows)
    square, part = expand(
        True, order, second_plan, second_plan[MISFIT, 0], kept_rows, kept_rows,
        square, sums, shifted(order, square), rows,
    )
    return divided(square, row_sums(part, rows))


def solution(mesh):
    in_specs = (P("pcol", "prow", None, None), P(), P(), P())
    out_specs = P("pcol", "prow", None, None)
    return jax.shard_map(local, mesh=mesh, in_specs=in_specs, out_specs=out_specs, check_vma=False)
```

```python
import functools

import jax
import jax.numpy as jnp
from jax import lax
from jax.experimental import pallas as pl
from jax.experimental.pallas import tpu as pltpu
from jax.sharding import PartitionSpec as P


SMEM = pl.BlockSpec(memory_space=pltpu.SMEM)
VMEM = pl.BlockSpec(memory_space=pltpu.VMEM)
ANY = pl.BlockSpec(memory_space=pl.ANY)

LANES = 128
SEND, FIRST, HOP, SECOND, MISFIT = range(5)
TILE_BIT, SENT_BIT = 4, 8


def ring(size, step):
    return [(i, (i + step) % size) for i in range(size)]


def row_sums(partial_value, size):
    sums = [partial_value]
    for step in range(1, size):
        sums.append(lax.ppermute(partial_value, "prow", ring(size, step)))
    return tuple(sums)


def plan_kernel(
    moved, steps, whole, order_ref, in_ref, out_ref, plan_ref, grid_ref, line_ref
):
    place, row = lax.axis_index("pcol"), lax.axis_index("prow")
    panels_all = order_ref.shape[1]
    depth = panels_all // 4
    share = in_ref.shape[0] // 4
    shape = (LANES, LANES)
    down = lax.broadcasted_iota(jnp.int32, shape, 0)
    along = lax.broadcasted_iota(jnp.int32, shape, 1)
    if moved:
        line_ref[...] = jnp.full(line_ref.shape, -2, jnp.int32)
        line_ref[:1, :panels_all] = order_ref[...]
        held = jnp.broadcast_to(line_ref[:1, :], shape)
    else:
        held = jnp.where(along < panels_all, along, -2)
    source = jnp.where(down < panels_all, down, -1)
    names = in_ref[...]
    panels, inside = names // 4, lax.rem(names, 4)
    groups = (down // 4 == held).astype(jnp.bfloat16)
    level, wide = lax.div(down, depth), lax.div(along, depth)
    same_level = level == wide
    valid = jnp.logical_and(down < depth * 4, along < depth * 4)
    spread = jnp.logical_and(
        jnp.logical_and(lax.rem(down, depth) == lax.rem(along, depth), valid),
        jnp.logical_not(same_level),
    ).astype(jnp.bfloat16)
    other = jnp.logical_and(valid, source != held)

    def product(left, right):
        return jnp.dot(
            left.astype(jnp.bfloat16), right.astype(jnp.bfloat16),
            preferred_element_type=jnp.float32,
        )

    def gathered(block):
        kept = [out_ref[pl.ds(block * share + t, 1), :] for t in range(share)]
        hits = []
        for u in range(share):
            line = jnp.broadcast_to(in_ref[pl.ds(block * share + u, 1), :], names.shape)
            value = jnp.take_along_axis(line, names, axis=1)
            hit = value == kept[0]
            for t in range(1, share):
                hit = jnp.logical_or(hit, value == kept[t])
            hits.append(hit.astype(jnp.float32))
        return hits

    def analyse(block):
        hits = gathered(block)
        zero = jnp.zeros(shape, jnp.float32)
        found, named, column = [zero] * share, zero, zero
        for k in range(names.shape[0]):
            here = (source == panels[k : k + 1, :]).astype(jnp.float32)
            named += here
            column += here * inside[k : k + 1, :].astype(jnp.float32)
            for u in range(share):
                found[u] += here * hits[u][k : k + 1, :]
        found = [jnp.where(other, product(value, groups), 0.0) > 0.5 for value in found]
        named = jnp.maximum(product(named, groups), 1.0)
        column = jnp.floor(product(column, groups) / named + 0.5)
        both = jnp.logical_and(found[0], found[1])
        away = jnp.logical_and(both, jnp.logical_not(same_level)).astype(jnp.float32)
        return found, column, both, away, product(away, spread)

    def fits():
        misfit = jnp.zeros(shape, jnp.float32)
        for block in range(4):
            found, _, both, away, riding = analyse(block)
            need = jnp.logical_or(found[0], found[1])
            crowded = jnp.logical_or(
                riding > 1.5, jnp.logical_and(riding > 0.5, jnp.logical_or(need, both))
            )
            misfit += jnp.where(
                jnp.logical_and(same_level, jnp.logical_or(crowded, both)), 1.0, 0.0
            )
            arriving = product(same_level.astype(jnp.float32), away)
            misfit += jnp.where(jnp.logical_and(valid, arriving > 1.5), 1.0, 0.0)
        total = jnp.sum(jnp.sum(misfit, axis=0, keepdims=True), axis=1, keepdims=True)
        line = jnp.broadcast_to((total > 0.5).astype(jnp.int32), (1, LANES))
        plan_ref[pl.ds(MISFIT, 1), :] = line

    if whole:
        fits()
    if steps is False:
        return

    found, column, both, away, riding = analyse(row)
    need = jnp.logical_or(found[0], found[1])
    direct = column + jnp.where(found[0], 0.0, float(TILE_BIT)) + SENT_BIT
    ride = product(away * column, spread) + TILE_BIT + SENT_BIT
    taken = jnp.logical_and(same_level, riding > 0.5)
    code = jnp.where(need, direct, jnp.where(taken, ride, 0.0))
    mine = (lax.broadcasted_iota(jnp.int32, (8, LANES), 1) == place).astype(jnp.float32)
    level_row = (
        lax.div(lax.broadcasted_iota(jnp.int32, (8, LANES), 1), depth) == lax.div(place, depth)
    ).astype(jnp.float32)
    first = lax.dot_general(
        mine.astype(jnp.bfloat16), found[0].astype(jnp.float32).astype(jnp.bfloat16),
        (((1,), (1,)), ((), ())), preferred_element_type=jnp.float32,
    )
    hop = product(level_row, away * (down + 1).astype(jnp.float32))
    grid_ref[0] = code
    grid_ref[1] = jnp.where(both, column + (TILE_BIT + SENT_BIT), 0.0)
    plan_ref[pl.ds(SEND, 1), :] = grid_ref[0, pl.ds(place, 1), :].astype(jnp.int32)
    plan_ref[pl.ds(FIRST, 1), :] = first[:1].astype(jnp.int32)
    plan_ref[pl.ds(HOP, 1), :] = hop[:1].astype(jnp.int32)
    plan_ref[pl.ds(SECOND, 1), :] = grid_ref[1, pl.ds(place, 1), :].astype(jnp.int32)


def plans_kernel(parts, order_ref, first_ref, second_ref, *rest):
    *plan_refs, grid_ref, line_ref = rest
    for (moved, steps, whole), plan_ref in zip(parts, plan_refs):
        in_ref = second_ref if moved else first_ref
        plan_kernel(
            moved, steps, whole, order_ref, in_ref, second_ref, plan_ref, grid_ref, line_ref
        )


def plans(parts, order_line, first_rows, second_rows):
    work = sum((1 if steps else 0) + (4 if whole else 0) for _, steps, whole in parts)
    return pl.pallas_call(
        functools.partial(plans_kernel, parts),
        out_shape=(jax.ShapeDtypeStruct((8, LANES), jnp.int32),) * len(parts),
        in_specs=[VMEM, VMEM, VMEM],
        out_specs=(VMEM,) * len(parts),
        scratch_shapes=[
            pltpu.VMEM((2, LANES, LANES), jnp.float32),
            pltpu.VMEM((8, LANES), jnp.int32),
        ],
        cost_estimate=pl.CostEstimate(
            flops=work << 23, bytes_accessed=1 << 14, transcendentals=0
        ),
    )(order_line, first_rows, second_rows)


def column_kernel(x_ref, part_ref):
    part_ref[...] = jnp.sum(x_ref[...], axis=(1, 2))


def column_partial(x):
    return pl.pallas_call(
        column_kernel,
        out_shape=jax.ShapeDtypeStruct((x.shape[0], x.shape[-1]), jnp.float32),
        in_specs=[VMEM],
        out_specs=VMEM,
        cost_estimate=pl.CostEstimate(flops=x.size, bytes_accessed=4 * x.size, transcendentals=0),
    )(x)


def send_kernel(line, plan_ref, x_ref, *rest):
    *sums, send_ref, normal, sems = rest
    panels = send_ref.shape[0]
    total = sums[0][...]
    for part in sums[1:]:
        total += part[...]
    normal[...] = x_ref[...] / total[:, None, None, :]

    def each(act):
        @pl.loop(0, panels)
        def _(slot):
            code = plan_ref[line, slot]

            @pl.when(code >= SENT_BIT)
            def _():
                tile = normal.at[code & 3, (code // TILE_BIT) & 1]
                act(pltpu.make_async_copy(tile, send_ref.at[slot], sems.at[slot]))

    each(lambda piece: piece.start())
    each(lambda piece: piece.wait())


def prepare(line, steps, x, sums, panels):
    tile = x.shape[-1]
    return pl.pallas_call(
        functools.partial(send_kernel, line),
        out_shape=jax.ShapeDtypeStruct((panels, tile, tile), jnp.float32),
        in_specs=[SMEM, VMEM] + [VMEM] * len(sums),
        out_specs=ANY,
        scratch_shapes=[
            pltpu.VMEM(x.shape, jnp.float32),
            pltpu.SemaphoreType.DMA((panels,)),
        ],
        cost_estimate=pl.CostEstimate(flops=x.size, bytes_accessed=3 << 20, transcendentals=0),
    )(steps, x, *sums)


def hop_kernel(plan_ref, got_ref, *rest):
    *outs, sems = rest
    place = lax.axis_index("pcol")
    depth = got_ref.shape[0] // 4
    pieces = []
    for step, out in enumerate(outs):
        target = lax.rem(place + (step + 1) * depth, 4 * depth)
        slot = jnp.maximum(plan_ref[HOP, target] - 1, 0)
        pieces.append(pltpu.make_async_copy(got_ref.at[slot], out, sems.at[step]))
    for piece in pieces:
        piece.start()
    for piece in pieces:
        piece.wait()


def hop_tiles(steps, got):
    tile = jax.ShapeDtypeStruct(got.shape[1:], jnp.float32)
    return pl.pallas_call(
        hop_kernel,
        out_shape=(tile,) * 3,
        in_specs=[SMEM, ANY],
        out_specs=(VMEM,) * 3,
        scratch_shapes=[pltpu.SemaphoreType.DMA((3,))],
        cost_estimate=pl.CostEstimate(flops=0, bytes_accessed=6 << 16, transcendentals=0),
    )(steps, got)


def split(value):
    high = value.astype(jnp.bfloat16)
    low = (value - high.astype(jnp.float32)).astype(jnp.bfloat16)
    return high, low


def dot_exactly(left, right):
    left_high, left_low = split(left)
    right_high, right_low = split(right)
    dot = functools.partial(jnp.dot, preferred_element_type=jnp.float32)
    return (dot(left_low, right_high) + dot(left_high, right_low)) + dot(left_high, right_high)


FIRSTS, SECONDS, LIST = 2, 64, 128


def matched(in_ref, out_pat_ref, row, share, own_column, column, t):
    wanted = out_pat_ref[row * share + t, own_column]
    hit = wanted < 0
    at = 0
    for u in range(share):
        same = in_ref[row * share + u, column] == wanted
        hit = jnp.logical_or(hit, same)
        at = jnp.where(same, u, at)
    return hit, at


def held_panel(moved, order_ref):
    place = lax.axis_index("pcol")
    return order_ref[place] if moved else place


def list_kernel(moved, cols, share, order_ref, plan_ref, in_ref, out_pat_ref, list_ref):
    row = lax.axis_index("prow")
    panel = held_panel(moved, order_ref)
    names = in_ref.shape[0]

    def remote(place_of, counts):
        own_column = panel * cols + place_of // names
        column = in_ref[lax.rem(place_of, names), own_column]
        origin = column // cols
        firsts, seconds = counts
        for t in range(share):
            hit, at = matched(in_ref, out_pat_ref, row, share, own_column, column, t)
            hit = jnp.logical_and(hit, origin != panel)
            extra = jnp.logical_and(hit, jnp.logical_and(at == 1, plan_ref[FIRST, origin] > 0))
            simple = jnp.logical_and(hit, jnp.logical_not(extra))
            entry = (place_of * share + t) * 32 + origin

            @pl.when(simple)
            def _():
                list_ref[FIRSTS + firsts] = entry

            @pl.when(extra)
            def _():
                list_ref[SECONDS + seconds] = entry

            firsts = firsts + simple.astype(jnp.int32)
            seconds = seconds + extra.astype(jnp.int32)
        return firsts, seconds

    firsts, seconds = lax.fori_loop(0, cols * names, remote, (jnp.int32(0), jnp.int32(0)))
    list_ref[0] = firsts
    list_ref[1] = seconds


def tile_list(moved, cols, share, order, steps, in_pattern, out_pattern):
    return pl.pallas_call(
        functools.partial(list_kernel, moved, cols, share),
        out_shape=jax.ShapeDtypeStruct((LIST,), jnp.int32),
        in_specs=[SMEM] * 4,
        out_specs=SMEM,
        cost_estimate=pl.CostEstimate(flops=1 << 28, bytes_accessed=1 << 14, transcendentals=0),
    )(order, steps, in_pattern, out_pattern)


def own_kernel(
    moved, order_ref, in_ref, out_pat_ref,
    own_ref, ahead_ref, behind_ref, far_low_ref, far_high_ref,
    base_ref, totals_ref, right_ref,
):
    cols, share, tile, _ = own_ref.shape
    row = lax.axis_index("prow")
    rows = in_ref.shape[0] // share
    panel = held_panel(moved, order_ref)
    home = panel // (order_ref.shape[0] // rows)
    half = cols // 2

    def piece(rel, j):
        far = far_low_ref.at[j] if j < half else far_high_ref.at[j - half]
        return (own_ref.at[j], ahead_ref.at[j], far, behind_ref.at[j])[rel]

    for j in range(cols):
        total = jnp.zeros((1, tile), jnp.float32)
        for rel in range(rows):
            whole = piece(rel, j)[...].reshape(share * tile, tile)
            total += jnp.sum(whole, axis=0, keepdims=True)
        totals_ref[pl.ds(j, 1), :] = total
    for rel in range(rows):

        @pl.when(lax.rem(row + rel, rows) == home)
        def _():
            for j in range(cols):
                right_ref[j] = piece(rel, j)[...]

    @pl.loop(0, cols)
    def _(j):
        base_ref[j] = jnp.zeros((share, tile, tile), jnp.float32)
        for s in range(share):
            own_column = panel * cols + j
            column = in_ref[home * share + s, own_column]
            local = lax.rem(column, cols)
            for t in range(share):
                hit, at = matched(in_ref, out_pat_ref, row, share, own_column, column, t)

                @pl.when(jnp.logical_and(hit, column // cols == panel))
                def _():
                    left = own_ref[local, at] / totals_ref[pl.ds(local, 1), :]
                    base_ref[j, t] += dot_exactly(left, right_ref[j, s])


def own_products(moved, order, in_pattern, out_pattern, pieces):
    own = pieces[0]
    cols, _, tile, _ = own.shape
    return pl.pallas_call(
        functools.partial(own_kernel, moved),
        out_shape=(
            jax.ShapeDtypeStruct(own.shape, jnp.float32),
            jax.ShapeDtypeStruct((cols, tile), jnp.float32),
        ),
        in_specs=[SMEM] * 3 + [VMEM] * 5,
        out_specs=(VMEM, VMEM),
        scratch_shapes=[pltpu.VMEM(own.shape, jnp.float32)],
        cost_estimate=pl.CostEstimate(flops=1 << 26, bytes_accessed=3 << 20, transcendentals=0),
    )(order, in_pattern, out_pattern, *pieces)


def pick_kernel(order_ref, held_ref, below_ref, above_ref, out_ref, sem):
    place = lax.axis_index("pcol")
    panel = order_ref[place]
    for chosen, ref in (
        (panel == place, held_ref), (panel < place, below_ref), (panel > place, above_ref)
    ):

        @pl.when(chosen)
        def _():
            pltpu.make_async_copy(ref, out_ref, sem).start()

    pltpu.make_async_copy(held_ref, out_ref, sem).wait()


def shifted(order, x):
    up = [(i, i + 1) for i in range(order.shape[0] - 1)]
    from_below = lax.ppermute(x, "pcol", up)
    from_above = lax.ppermute(x, "pcol", [(j, i) for i, j in up])
    return pl.pallas_call(
        pick_kernel,
        out_shape=jax.ShapeDtypeStruct(x.shape, jnp.float32),
        in_specs=[SMEM, ANY, ANY, ANY],
        out_specs=VMEM,
        scratch_shapes=[pltpu.SemaphoreType.DMA],
        cost_estimate=pl.CostEstimate(flops=0, bytes_accessed=1 << 20, transcendentals=0),
    )(order, x, from_below, from_above)


def add_listed(list_ref, number, first, right_refs, acc_ref, fetch, lefts, rights, sems):
    own_ref, ahead_ref, behind_ref, far_low_ref, far_high_ref = right_refs
    row, rows = lax.axis_index("prow"), lax.axis_size("prow")
    share = acc_ref.shape[1]
    names = rows * share
    half = far_low_ref.shape[0]
    count = list_ref[number]

    def where(i):
        entry = list_ref[first + i]
        spot = entry // 32
        column_slot = spot // share
        return (
            column_slot // names, lax.rem(column_slot, names), lax.rem(spot, share),
            lax.rem(entry, 32),
        )

    def wait_for(which, buffers, i):
        pltpu.make_async_copy(own_ref.at[0, 0], buffers.at[i], sems.at[which, i]).wait()

    @pl.loop(0, count)
    def _(i):
        j, k, _, origin = where(i)
        fetch(i, origin)
        rel = lax.rem(k // share - row + rows, rows)
        s = lax.rem(k, share)
        low = j < half
        for chosen, ref, at in (
            (rel == 0, own_ref, j), (rel == 1, ahead_ref, j), (rel == 3, behind_ref, j),
            (jnp.logical_and(rel == 2, low), far_low_ref, j),
            (jnp.logical_and(rel == 2, jnp.logical_not(low)), far_high_ref, j - half),
        ):

            @pl.when(chosen)
            def _():
                pltpu.make_async_copy(ref.at[at, s], rights.at[i], sems.at[1, i]).start()

    @pl.loop(0, count)
    def _(i):
        j, _, t, _ = where(i)
        wait_for(1, rights, i)
        wait_for(0, lefts, i)
        acc_ref[j, t] += dot_exactly(lefts[i], rights[i])


def main_kernel(list_ref, base_ref, got_ref, *rest):
    *right_refs, acc_ref, lefts, rights, sems = rest
    acc_ref[...] = base_ref[...]

    def fetch(i, origin):
        pltpu.make_async_copy(got_ref.at[origin], lefts.at[i], sems.at[0, i]).start()

    add_listed(list_ref, 0, FIRSTS, right_refs, acc_ref, fetch, lefts, rights, sems)


def last_kernel(depth, list_ref, acc_in_ref, totals_ref, *rest):
    right_refs = rest[:5]
    *extra_refs, sq_ref, part_ref, lefts, rights, sems = rest[5:]
    cols, share, tile, _ = acc_in_ref.shape
    place = lax.axis_index("pcol")
    sq_ref[...] = acc_in_ref[...]

    def fetch(i, origin):
        if len(extra_refs) == 1:
            pltpu.make_async_copy(extra_refs[0].at[origin], lefts.at[i], sems.at[0, i]).start()
            return
        step = lax.rem(place // depth - origin // depth + 4, 4)
        for distance, ref in enumerate(extra_refs):

            @pl.when(step == distance + 1)
            def _():
                pltpu.make_async_copy(ref, lefts.at[i], sems.at[0, i]).start()

    add_listed(list_ref, 1, SECONDS, right_refs, sq_ref, fetch, lefts, rights, sems)
    for j in range(cols):
        value = sq_ref[j].reshape(share * tile, tile) / totals_ref[pl.ds(j, 1), :]
        square = value * value
        sq_ref[j] = square.reshape(share, tile, tile)
        part_ref[pl.ds(j, 1), :] = jnp.sum(square, axis=0, keepdims=True)


def list_scratch(tile):
    most = SECONDS - FIRSTS - 2
    return [
        pltpu.VMEM((most, tile, tile), jnp.float32),
        pltpu.VMEM((most, tile, tile), jnp.float32),
        pltpu.SemaphoreType.DMA((2, most)),
    ]


def main_products(tiles, base, pieces, got):
    return pl.pallas_call(
        main_kernel,
        out_shape=jax.ShapeDtypeStruct(base.shape, jnp.float32),
        in_specs=[SMEM, VMEM, ANY] + [ANY] * 5,
        out_specs=VMEM,
        scratch_shapes=list_scratch(base.shape[-1]),
        cost_estimate=pl.CostEstimate(flops=1 << 30, bytes_accessed=3 << 20, transcendentals=0),
    )(tiles, base, got, *pieces)


def last_products(depth, tiles, acc, totals, pieces, extra):
    cols, _, tile, _ = acc.shape
    return pl.pallas_call(
        functools.partial(last_kernel, depth),
        out_shape=(
            jax.ShapeDtypeStruct(acc.shape, jnp.float32),
            jax.ShapeDtypeStruct((cols, tile), jnp.float32),
        ),
        in_specs=[SMEM, VMEM, VMEM] + [ANY] * (5 + len(extra)),
        out_specs=(VMEM, VMEM),
        scratch_shapes=list_scratch(tile),
        cost_estimate=pl.CostEstimate(flops=1 << 24, bytes_accessed=2 << 20, transcendentals=0),
    )(tiles, acc, totals, *pieces, *extra)


def divide_kernel(x_ref, *rest):
    *sums, out_ref = rest
    total = sums[0][...]
    for part in sums[1:]:
        total += part[...]
    out_ref[...] = x_ref[...] / total[:, None, None, :]


def divided(x, sums):
    return pl.pallas_call(
        divide_kernel,
        out_shape=jax.ShapeDtypeStruct(x.shape, jnp.float32),
        in_specs=[VMEM] * (1 + len(sums)),
        out_specs=VMEM,
        cost_estimate=pl.CostEstimate(flops=x.size, bytes_accessed=1 << 20, transcendentals=0),
    )(x, *sums)


def gather_rows(own, size):
    half = own.shape[0] // 2
    behind = lax.ppermute(own, "prow", ring(size, 1))
    ahead = lax.ppermute(own, "prow", ring(size, -1))
    far_low = lax.ppermute(behind[:half], "prow", ring(size, 1))
    far_high = lax.ppermute(ahead[half:], "prow", ring(size, -1))
    return ahead, behind, far_low, far_high


def expand(moved, order, steps, misfit, in_pattern, out_pattern, x, sums, own, rows):
    cols, share = x.shape[:2]
    panels = order.shape[0]
    depth = panels // 4
    send = prepare(SEND, steps, x, sums, panels)
    got = lax.all_to_all(send, "pcol", 0, 0, tiled=True)
    tiles = tile_list(moved, cols, share, order, steps, in_pattern, out_pattern)
    pieces = (own,) + gather_rows(own, rows)
    base, totals = own_products(moved, order, in_pattern, out_pattern, pieces)

    def by_level(_):
        hops = hop_tiles(steps, got)
        extra = tuple(
            lax.ppermute(tile, "pcol", ring(panels, (step + 1) * depth))
            for step, tile in enumerate(hops)
        )
        acc = main_products(tiles, base, pieces, got)
        return last_products(depth, tiles, acc, totals, pieces, extra)

    def by_second(_):
        more = prepare(SECOND, steps, x, sums, panels)
        extra = (lax.all_to_all(more, "pcol", 0, 0, tiled=True),)
        acc = main_products(tiles, base, pieces, got)
        return last_products(depth, tiles, acc, totals, pieces, extra)

    return lax.cond(misfit > 0, by_second, by_level, 0)


def local(match_tiles, pattern, kept, panel_order):
    rows = lax.axis_size("prow")
    order = panel_order
    pattern_rows = pattern.T
    kept_rows = kept.T
    tables = (order[None], pattern_rows, kept_rows)
    (first_plan,) = plans(((False, True, False),), *tables)
    sums = row_sums(column_partial(match_tiles), rows)
    check, second_plan = plans(((False, False, True), (True, True, True)), *tables)
    square, part = expand(
        False, order, first_plan, check[MISFIT, 0], pattern_rows, kept_rows,
        match_tiles, sums, match_tiles, rows,
    )
    sums = row_sums(part, rows)
    square, part = expand(
        True, order, second_plan, second_plan[MISFIT, 0], kept_rows, kept_rows,
        square, sums, shifted(order, square), rows,
    )
    return divided(square, row_sums(part, rows))


def solution(mesh):
    in_specs = (P("pcol", "prow", None, None), P(), P(), P())
    out_specs = P("pcol", "prow", None, None)
    return jax.shard_map(local, mesh=mesh, in_specs=in_specs, out_specs=out_specs, check_vma=False)
```

```python
import functools

import jax
import jax.numpy as jnp
from jax import lax
from jax.experimental import pallas as pl
from jax.experimental.pallas import tpu as pltpu
from jax.sharding import PartitionSpec as P


SMEM = pl.BlockSpec(memory_space=pltpu.SMEM)
VMEM = pl.BlockSpec(memory_space=pltpu.VMEM)
ANY = pl.BlockSpec(memory_space=pl.ANY)

LANES = 128
SEND, FIRST, HOP, SECOND, MISFIT = range(5)
TILE_BIT, SENT_BIT = 4, 8


def ring(size, step):
    return [(i, (i + step) % size) for i in range(size)]


def row_sums(partial_value, size):
    sums = [partial_value]
    for step in range(1, size):
        sums.append(lax.ppermute(partial_value, "prow", ring(size, step)))
    return tuple(sums)


def plan_kernel(
    permuted, steps, whole, order_ref, in_ref, out_ref, plan_ref, grid_ref, line_ref
):
    place, row = lax.axis_index("pcol"), lax.axis_index("prow")
    panels_all = order_ref.shape[1]
    depth = panels_all // 4
    share = in_ref.shape[0] // 4
    shape = (LANES, LANES)
    down = lax.broadcasted_iota(jnp.int32, shape, 0)
    along = lax.broadcasted_iota(jnp.int32, shape, 1)
    line_ref[...] = jnp.full(line_ref.shape, -2, jnp.int32)
    line_ref[:1, :panels_all] = order_ref[...]
    held = jnp.broadcast_to(line_ref[:1, :], shape)
    if permuted:
        diagonal = jnp.where(down == along, held, 0)
        source = jnp.broadcast_to(jnp.sum(diagonal, axis=1, keepdims=True), shape)
        source = jnp.where(down < panels_all, source, -1)
    else:
        source = jnp.where(down < panels_all, down, -1)
    names = in_ref[...]
    panels, inside = names // 4, lax.rem(names, 4)
    groups = (down // 4 == held).astype(jnp.bfloat16)
    level, wide = lax.div(down, depth), lax.div(along, depth)
    same_level = level == wide
    valid = jnp.logical_and(down < depth * 4, along < depth * 4)
    spread = jnp.logical_and(
        jnp.logical_and(lax.rem(down, depth) == lax.rem(along, depth), valid),
        jnp.logical_not(same_level),
    ).astype(jnp.bfloat16)
    other = jnp.logical_and(valid, source != held)

    def product(left, right):
        return jnp.dot(
            left.astype(jnp.bfloat16), right.astype(jnp.bfloat16),
            preferred_element_type=jnp.float32,
        )

    def gathered(block):
        kept = [out_ref[pl.ds(block * share + t, 1), :] for t in range(share)]
        hits = []
        for u in range(share):
            line = jnp.broadcast_to(in_ref[pl.ds(block * share + u, 1), :], names.shape)
            value = jnp.take_along_axis(line, names, axis=1)
            hit = value == kept[0]
            for t in range(1, share):
                hit = jnp.logical_or(hit, value == kept[t])
            hits.append(hit.astype(jnp.float32))
        return hits

    def analyse(block):
        hits = gathered(block)
        zero = jnp.zeros(shape, jnp.float32)
        found, named, column = [zero] * share, zero, zero
        for k in range(names.shape[0]):
            here = (source == panels[k : k + 1, :]).astype(jnp.float32)
            named += here
            column += here * inside[k : k + 1, :].astype(jnp.float32)
            for u in range(share):
                found[u] += here * hits[u][k : k + 1, :]
        found = [jnp.where(other, product(value, groups), 0.0) > 0.5 for value in found]
        named = jnp.maximum(product(named, groups), 1.0)
        column = jnp.floor(product(column, groups) / named + 0.5)
        both = jnp.logical_and(found[0], found[1])
        away = jnp.logical_and(both, jnp.logical_not(same_level)).astype(jnp.float32)
        return found, column, both, away, product(away, spread)

    def fits():
        misfit = jnp.zeros(shape, jnp.float32)
        for block in range(4):
            found, _, both, away, riding = analyse(block)
            need = jnp.logical_or(found[0], found[1])
            crowded = jnp.logical_or(
                riding > 1.5, jnp.logical_and(riding > 0.5, jnp.logical_or(need, both))
            )
            misfit += jnp.where(
                jnp.logical_and(same_level, jnp.logical_or(crowded, both)), 1.0, 0.0
            )
            arriving = product(same_level.astype(jnp.float32), away)
            misfit += jnp.where(jnp.logical_and(valid, arriving > 1.5), 1.0, 0.0)
        total = jnp.sum(jnp.sum(misfit, axis=0, keepdims=True), axis=1, keepdims=True)
        line = jnp.broadcast_to((total > 0.5).astype(jnp.int32), (1, LANES))
        plan_ref[pl.ds(MISFIT, 1), :] = line

    if whole:
        fits()
    if steps is False:
        return

    found, column, both, away, riding = analyse(row)
    need = jnp.logical_or(found[0], found[1])
    direct = column + jnp.where(found[0], 0.0, float(TILE_BIT)) + SENT_BIT
    ride = product(away * column, spread) + TILE_BIT + SENT_BIT
    taken = jnp.logical_and(same_level, riding > 0.5)
    code = jnp.where(need, direct, jnp.where(taken, ride, 0.0))
    mine = (lax.broadcasted_iota(jnp.int32, (8, LANES), 1) == place).astype(jnp.float32)
    level_row = (
        lax.div(lax.broadcasted_iota(jnp.int32, (8, LANES), 1), depth) == lax.div(place, depth)
    ).astype(jnp.float32)
    first = lax.dot_general(
        mine.astype(jnp.bfloat16), found[0].astype(jnp.float32).astype(jnp.bfloat16),
        (((1,), (1,)), ((), ())), preferred_element_type=jnp.float32,
    )
    hop = product(level_row, away * (down + 1).astype(jnp.float32))
    grid_ref[0] = code
    grid_ref[1] = jnp.where(both, column + (TILE_BIT + SENT_BIT), 0.0)
    plan_ref[pl.ds(SEND, 1), :] = grid_ref[0, pl.ds(place, 1), :].astype(jnp.int32)
    plan_ref[pl.ds(FIRST, 1), :] = first[:1].astype(jnp.int32)
    plan_ref[pl.ds(HOP, 1), :] = hop[:1].astype(jnp.int32)
    plan_ref[pl.ds(SECOND, 1), :] = grid_ref[1, pl.ds(place, 1), :].astype(jnp.int32)


def plans_kernel(parts, order_ref, first_ref, second_ref, *rest):
    *plan_refs, grid_ref, line_ref = rest
    for (permuted, steps, whole), plan_ref in zip(parts, plan_refs):
        in_ref = second_ref if permuted else first_ref
        plan_kernel(
            permuted, steps, whole, order_ref, in_ref, second_ref, plan_ref, grid_ref, line_ref
        )


def plans(parts, order_line, first_rows, second_rows):
    work = sum((1 if steps else 0) + (4 if whole else 0) for _, steps, whole in parts)
    return pl.pallas_call(
        functools.partial(plans_kernel, parts),
        out_shape=(jax.ShapeDtypeStruct((8, LANES), jnp.int32),) * len(parts),
        in_specs=[VMEM, VMEM, VMEM],
        out_specs=(VMEM,) * len(parts),
        scratch_shapes=[
            pltpu.VMEM((2, LANES, LANES), jnp.float32),
            pltpu.VMEM((8, LANES), jnp.int32),
        ],
        cost_estimate=pl.CostEstimate(
            flops=work << 23, bytes_accessed=1 << 14, transcendentals=0
        ),
    )(order_line, first_rows, second_rows)


def column_kernel(x_ref, part_ref):
    part_ref[...] = jnp.sum(x_ref[...], axis=(1, 2))


def column_partial(x):
    return pl.pallas_call(
        column_kernel,
        out_shape=jax.ShapeDtypeStruct((x.shape[0], x.shape[-1]), jnp.float32),
        in_specs=[VMEM],
        out_specs=VMEM,
        cost_estimate=pl.CostEstimate(flops=x.size, bytes_accessed=4 * x.size, transcendentals=0),
    )(x)


def send_kernel(line, plan_ref, x_ref, *rest):
    *sums, send_ref, normal, sems = rest
    panels = send_ref.shape[0]
    total = sums[0][...]
    for part in sums[1:]:
        total += part[...]
    normal[...] = x_ref[...] / total[:, None, None, :]

    def each(act):
        @pl.loop(0, panels)
        def _(slot):
            code = plan_ref[line, slot]

            @pl.when(code >= SENT_BIT)
            def _():
                tile = normal.at[code & 3, (code // TILE_BIT) & 1]
                act(pltpu.make_async_copy(tile, send_ref.at[slot], sems.at[slot]))

    each(lambda piece: piece.start())
    each(lambda piece: piece.wait())


def prepare(line, steps, x, sums, panels):
    tile = x.shape[-1]
    return pl.pallas_call(
        functools.partial(send_kernel, line),
        out_shape=jax.ShapeDtypeStruct((panels, tile, tile), jnp.float32),
        in_specs=[SMEM, VMEM] + [VMEM] * len(sums),
        out_specs=ANY,
        scratch_shapes=[
            pltpu.VMEM(x.shape, jnp.float32),
            pltpu.SemaphoreType.DMA((panels,)),
        ],
        cost_estimate=pl.CostEstimate(flops=x.size, bytes_accessed=3 << 20, transcendentals=0),
    )(steps, x, *sums)


def hop_kernel(plan_ref, got_ref, *rest):
    *outs, sems = rest
    place = lax.axis_index("pcol")
    depth = got_ref.shape[0] // 4
    pieces = []
    for step, out in enumerate(outs):
        target = lax.rem(place + (step + 1) * depth, 4 * depth)
        slot = jnp.maximum(plan_ref[HOP, target] - 1, 0)
        pieces.append(pltpu.make_async_copy(got_ref.at[slot], out, sems.at[step]))
    for piece in pieces:
        piece.start()
    for piece in pieces:
        piece.wait()


def hop_tiles(steps, got):
    tile = jax.ShapeDtypeStruct(got.shape[1:], jnp.float32)
    return pl.pallas_call(
        hop_kernel,
        out_shape=(tile,) * 3,
        in_specs=[SMEM, ANY],
        out_specs=(VMEM,) * 3,
        scratch_shapes=[pltpu.SemaphoreType.DMA((3,))],
        cost_estimate=pl.CostEstimate(flops=0, bytes_accessed=6 << 16, transcendentals=0),
    )(steps, got)


def split(value):
    high = value.astype(jnp.bfloat16)
    low = (value - high.astype(jnp.float32)).astype(jnp.bfloat16)
    return high, low


def dot_exactly(left, right):
    left_high, left_low = split(left)
    right_high, right_low = split(right)
    dot = functools.partial(jnp.dot, preferred_element_type=jnp.float32)
    return (dot(left_low, right_high) + dot(left_high, right_low)) + dot(left_high, right_high)


FIRSTS, SECONDS, LIST = 2, 64, 128


def matched(in_ref, out_pat_ref, row, share, own_column, column, t):
    wanted = out_pat_ref[row * share + t, own_column]
    hit = wanted < 0
    at = 0
    for u in range(share):
        same = in_ref[row * share + u, column] == wanted
        hit = jnp.logical_or(hit, same)
        at = jnp.where(same, u, at)
    return hit, at


def list_kernel(permuted, cols, share, order_ref, plan_ref, in_ref, out_pat_ref, list_ref):
    row = lax.axis_index("prow")
    panel = order_ref[lax.axis_index("pcol")]
    names = in_ref.shape[0]

    def remote(place_of, counts):
        own_column = panel * cols + place_of // names
        column = in_ref[lax.rem(place_of, names), own_column]
        source = column // cols
        origin = order_ref[source] if permuted else source
        firsts, seconds = counts
        for t in range(share):
            hit, at = matched(in_ref, out_pat_ref, row, share, own_column, column, t)
            hit = jnp.logical_and(hit, source != panel)
            extra = jnp.logical_and(hit, jnp.logical_and(at == 1, plan_ref[FIRST, origin] > 0))
            simple = jnp.logical_and(hit, jnp.logical_not(extra))
            entry = (place_of * share + t) * 32 + origin

            @pl.when(simple)
            def _():
                list_ref[FIRSTS + firsts] = entry

            @pl.when(extra)
            def _():
                list_ref[SECONDS + seconds] = entry

            firsts = firsts + simple.astype(jnp.int32)
            seconds = seconds + extra.astype(jnp.int32)
        return firsts, seconds

    firsts, seconds = lax.fori_loop(0, cols * names, remote, (jnp.int32(0), jnp.int32(0)))
    list_ref[0] = firsts
    list_ref[1] = seconds


def tile_list(permuted, cols, share, order, steps, in_pattern, out_pattern):
    return pl.pallas_call(
        functools.partial(list_kernel, permuted, cols, share),
        out_shape=jax.ShapeDtypeStruct((LIST,), jnp.int32),
        in_specs=[SMEM] * 4,
        out_specs=SMEM,
        cost_estimate=pl.CostEstimate(flops=1 << 28, bytes_accessed=1 << 14, transcendentals=0),
    )(order, steps, in_pattern, out_pattern)


def own_kernel(
    order_ref, in_ref, out_pat_ref,
    own_ref, ahead_ref, behind_ref, far_low_ref, far_high_ref,
    base_ref, totals_ref, right_ref,
):
    cols, share, tile, _ = own_ref.shape
    row = lax.axis_index("prow")
    rows = right_ref.shape[1] // share
    panel = order_ref[lax.axis_index("pcol")]
    home = panel // (order_ref.shape[0] // rows)
    half = cols // 2

    for rel in range(4):
        first = lax.rem(row + rel, rows) * share
        for j in range(cols):
            far = far_low_ref.at[j] if j < half else far_high_ref.at[j - half]
            piece = (own_ref.at[j], ahead_ref.at[j], far, behind_ref.at[j])[rel]
            right_ref[j, pl.ds(first, share)] = piece[...]
    for j in range(cols):
        whole = right_ref[j].reshape(rows * share * tile, tile)
        totals_ref[pl.ds(j, 1), :] = jnp.sum(whole, axis=0, keepdims=True)

    @pl.loop(0, cols)
    def _(j):
        base_ref[j] = jnp.zeros((share, tile, tile), jnp.float32)
        for s in range(share):
            k = home * share + s
            own_column = panel * cols + j
            column = in_ref[k, own_column]
            local = lax.rem(column, cols)
            for t in range(share):
                hit, at = matched(in_ref, out_pat_ref, row, share, own_column, column, t)

                @pl.when(jnp.logical_and(hit, column // cols == panel))
                def _():
                    left = own_ref[local, at] / totals_ref[pl.ds(local, 1), :]
                    base_ref[j, t] += dot_exactly(left, right_ref[j, k])


def own_products(order, in_pattern, out_pattern, own, gathered):
    cols, share, tile, _ = own.shape
    return pl.pallas_call(
        own_kernel,
        out_shape=(
            jax.ShapeDtypeStruct(own.shape, jnp.float32),
            jax.ShapeDtypeStruct((cols, tile), jnp.float32),
            jax.ShapeDtypeStruct((cols, 4 * share, tile, tile), jnp.float32),
        ),
        in_specs=[SMEM] * 3 + [VMEM] * 5,
        out_specs=(VMEM, VMEM, VMEM),
        cost_estimate=pl.CostEstimate(flops=1 << 26, bytes_accessed=5 << 20, transcendentals=0),
    )(order, in_pattern, out_pattern, own, *gathered)


def pick_kernel(order_ref, held_ref, below_ref, above_ref, out_ref, sem):
    place = lax.axis_index("pcol")
    panel = order_ref[place]
    for chosen, ref in (
        (panel == place, held_ref), (panel < place, below_ref), (panel > place, above_ref)
    ):

        @pl.when(chosen)
        def _():
            pltpu.make_async_copy(ref, out_ref, sem).start()

    pltpu.make_async_copy(held_ref, out_ref, sem).wait()


def shifted(order, x):
    up = [(i, i + 1) for i in range(order.shape[0] - 1)]
    from_below = lax.ppermute(x, "pcol", up)
    from_above = lax.ppermute(x, "pcol", [(j, i) for i, j in up])
    return pl.pallas_call(
        pick_kernel,
        out_shape=jax.ShapeDtypeStruct(x.shape, jnp.float32),
        in_specs=[SMEM, ANY, ANY, ANY],
        out_specs=VMEM,
        scratch_shapes=[pltpu.SemaphoreType.DMA],
        cost_estimate=pl.CostEstimate(flops=0, bytes_accessed=1 << 20, transcendentals=0),
    )(order, x, from_below, from_above)


def add_listed(list_ref, number, first, right_ref, acc_ref, fetch, lefts, rights, sems):
    share = acc_ref.shape[1]
    names = right_ref.shape[1]
    count = list_ref[number]

    def where(i):
        entry = list_ref[first + i]
        spot = entry // 32
        column_slot = spot // share
        return (
            column_slot // names, lax.rem(column_slot, names), lax.rem(spot, share),
            lax.rem(entry, 32),
        )

    def right_copy(i, j, k):
        return pltpu.make_async_copy(right_ref.at[j, k], rights.at[i], sems.at[1, i])

    @pl.loop(0, count)
    def _(i):
        j, k, _, origin = where(i)
        right_copy(i, j, k).start()
        fetch(i, origin)

    @pl.loop(0, count)
    def _(i):
        j, k, t, _ = where(i)
        right_copy(i, j, k).wait()
        pltpu.make_async_copy(right_ref.at[j, k], lefts.at[i], sems.at[0, i]).wait()
        acc_ref[j, t] += dot_exactly(lefts[i], rights[i])


def main_kernel(list_ref, base_ref, right_ref, got_ref, acc_ref, lefts, rights, sems):
    acc_ref[...] = base_ref[...]

    def fetch(i, origin):
        pltpu.make_async_copy(got_ref.at[origin], lefts.at[i], sems.at[0, i]).start()

    add_listed(list_ref, 0, FIRSTS, right_ref, acc_ref, fetch, lefts, rights, sems)


def last_kernel(depth, list_ref, acc_in_ref, totals_ref, right_ref, *rest):
    *extra_refs, sq_ref, part_ref, lefts, rights, sems = rest
    cols, share, tile, _ = acc_in_ref.shape
    place = lax.axis_index("pcol")
    sq_ref[...] = acc_in_ref[...]

    def fetch(i, origin):
        if len(extra_refs) == 1:
            pltpu.make_async_copy(extra_refs[0].at[origin], lefts.at[i], sems.at[0, i]).start()
            return
        step = lax.rem(place // depth - origin // depth + 4, 4)
        for distance, ref in enumerate(extra_refs):

            @pl.when(step == distance + 1)
            def _():
                pltpu.make_async_copy(ref, lefts.at[i], sems.at[0, i]).start()

    add_listed(list_ref, 1, SECONDS, right_ref, sq_ref, fetch, lefts, rights, sems)
    for j in range(cols):
        value = sq_ref[j].reshape(share * tile, tile) / totals_ref[pl.ds(j, 1), :]
        square = value * value
        sq_ref[j] = square.reshape(share, tile, tile)
        part_ref[pl.ds(j, 1), :] = jnp.sum(square, axis=0, keepdims=True)


def list_scratch(right):
    _, _, tile, _ = right.shape
    most = SECONDS - FIRSTS - 2
    return [
        pltpu.VMEM((most, tile, tile), jnp.float32),
        pltpu.VMEM((most, tile, tile), jnp.float32),
        pltpu.SemaphoreType.DMA((2, most)),
    ]


def main_products(tiles, base, right, got):
    return pl.pallas_call(
        main_kernel,
        out_shape=jax.ShapeDtypeStruct(base.shape, jnp.float32),
        in_specs=[SMEM, VMEM, ANY, ANY],
        out_specs=VMEM,
        scratch_shapes=list_scratch(right),
        cost_estimate=pl.CostEstimate(flops=1 << 30, bytes_accessed=3 << 20, transcendentals=0),
    )(tiles, base, right, got)


def last_products(depth, tiles, acc, totals, right, extra):
    cols, _, tile, _ = acc.shape
    return pl.pallas_call(
        functools.partial(last_kernel, depth),
        out_shape=(
            jax.ShapeDtypeStruct(acc.shape, jnp.float32),
            jax.ShapeDtypeStruct((cols, tile), jnp.float32),
        ),
        in_specs=[SMEM, VMEM, VMEM, ANY] + [ANY] * len(extra),
        out_specs=(VMEM, VMEM),
        scratch_shapes=list_scratch(right),
        cost_estimate=pl.CostEstimate(flops=1 << 24, bytes_accessed=2 << 20, transcendentals=0),
    )(tiles, acc, totals, right, *extra)


def divide_kernel(x_ref, *rest):
    *sums, out_ref = rest
    total = sums[0][...]
    for part in sums[1:]:
        total += part[...]
    out_ref[...] = x_ref[...] / total[:, None, None, :]


def divided(x, sums):
    return pl.pallas_call(
        divide_kernel,
        out_shape=jax.ShapeDtypeStruct(x.shape, jnp.float32),
        in_specs=[VMEM] * (1 + len(sums)),
        out_specs=VMEM,
        cost_estimate=pl.CostEstimate(flops=x.size, bytes_accessed=1 << 20, transcendentals=0),
    )(x, *sums)


def gather_rows(own, size):
    half = own.shape[0] // 2
    behind = lax.ppermute(own, "prow", ring(size, 1))
    ahead = lax.ppermute(own, "prow", ring(size, -1))
    far_low = lax.ppermute(behind[:half], "prow", ring(size, 1))
    far_high = lax.ppermute(ahead[half:], "prow", ring(size, -1))
    return ahead, behind, far_low, far_high


def expand(permuted, order, steps, misfit, in_pattern, out_pattern, x, sums, own, rows):
    cols, share = x.shape[:2]
    panels = order.shape[0]
    depth = panels // 4
    send = prepare(SEND, steps, x, sums, panels)
    got = lax.all_to_all(send, "pcol", 0, 0, tiled=True)
    tiles = tile_list(permuted, cols, share, order, steps, in_pattern, out_pattern)
    gathered = gather_rows(own, rows)
    base, totals, right = own_products(order, in_pattern, out_pattern, own, gathered)

    def by_level(_):
        hops = hop_tiles(steps, got)
        extra = tuple(
            lax.ppermute(tile, "pcol", ring(panels, (step + 1) * depth))
            for step, tile in enumerate(hops)
        )
        acc = main_products(tiles, base, right, got)
        return last_products(depth, tiles, acc, totals, right, extra)

    def by_second(_):
        more = prepare(SECOND, steps, x, sums, panels)
        extra = (lax.all_to_all(more, "pcol", 0, 0, tiled=True),)
        acc = main_products(tiles, base, right, got)
        return last_products(depth, tiles, acc, totals, right, extra)

    return lax.cond(misfit > 0, by_second, by_level, 0)


def local(match_tiles, pattern, kept, panel_order):
    rows = lax.axis_size("prow")
    order = panel_order
    pattern_rows = pattern.T
    kept_rows = kept.T
    tables = (order[None], pattern_rows, kept_rows)
    (first_plan,) = plans(((False, True, False),), *tables)
    sums = row_sums(column_partial(match_tiles), rows)
    check, second_plan = plans(((False, False, True), (True, True, True)), *tables)
    square, part = expand(
        False, order, first_plan, check[MISFIT, 0], pattern_rows, kept_rows,
        match_tiles, sums, shifted(order, match_tiles), rows,
    )
    sums = row_sums(part, rows)
    square, part = expand(
        True, order, second_plan, second_plan[MISFIT, 0], kept_rows, kept_rows,
        square, sums, square, rows,
    )
    return divided(square, row_sums(part, rows))


def solution(mesh):
    in_specs = (P("pcol", "prow", None, None), P(), P(), P())
    out_specs = P("pcol", "prow", None, None)
    return jax.shard_map(local, mesh=mesh, in_specs=in_specs, out_specs=out_specs, check_vma=False)
```

```python
import functools

import jax
import jax.numpy as jnp
from jax import lax
from jax.experimental import pallas as pl
from jax.experimental.pallas import tpu as pltpu
from jax.sharding import PartitionSpec as P


SMEM = pl.BlockSpec(memory_space=pltpu.SMEM)
VMEM = pl.BlockSpec(memory_space=pltpu.VMEM)
ANY = pl.BlockSpec(memory_space=pl.ANY)

LANES = 128
SEND, FIRST, HOP, SECOND, MISFIT = range(5)
TILE_BIT, SENT_BIT = 4, 8


def ring(size, step):
    return [(i, (i + step) % size) for i in range(size)]


def row_sums(partial_value, size):
    sums = [partial_value]
    for step in range(1, size):
        sums.append(lax.ppermute(partial_value, "prow", ring(size, step)))
    return tuple(sums)


def plan_kernel(
    permuted, steps, whole, order_ref, in_ref, out_ref, plan_ref, grid_ref, line_ref
):
    place, row = lax.axis_index("pcol"), lax.axis_index("prow")
    panels_all = order_ref.shape[1]
    depth = panels_all // 4
    share = in_ref.shape[0] // 4
    shape = (LANES, LANES)
    down = lax.broadcasted_iota(jnp.int32, shape, 0)
    along = lax.broadcasted_iota(jnp.int32, shape, 1)
    line_ref[...] = jnp.full(line_ref.shape, -2, jnp.int32)
    line_ref[:1, :panels_all] = order_ref[...]
    held = jnp.broadcast_to(line_ref[:1, :], shape)
    if permuted:
        diagonal = jnp.where(down == along, held, 0)
        source = jnp.broadcast_to(jnp.sum(diagonal, axis=1, keepdims=True), shape)
        source = jnp.where(down < panels_all, source, -1)
    else:
        source = jnp.where(down < panels_all, down, -1)
    names = in_ref[...]
    panels, inside = names // 4, lax.rem(names, 4)
    groups = (down // 4 == held).astype(jnp.bfloat16)
    level, wide = lax.div(down, depth), lax.div(along, depth)
    same_level = level == wide
    valid = jnp.logical_and(down < depth * 4, along < depth * 4)
    spread = jnp.logical_and(
        jnp.logical_and(lax.rem(down, depth) == lax.rem(along, depth), valid),
        jnp.logical_not(same_level),
    ).astype(jnp.bfloat16)
    other = jnp.logical_and(valid, source != held)

    def product(left, right):
        return jnp.dot(
            left.astype(jnp.bfloat16), right.astype(jnp.bfloat16),
            preferred_element_type=jnp.float32,
        )

    def gathered(block):
        kept = [out_ref[pl.ds(block * share + t, 1), :] for t in range(share)]
        hits = []
        for u in range(share):
            line = jnp.broadcast_to(in_ref[pl.ds(block * share + u, 1), :], names.shape)
            value = jnp.take_along_axis(line, names, axis=1)
            hit = value == kept[0]
            for t in range(1, share):
                hit = jnp.logical_or(hit, value == kept[t])
            hits.append(hit.astype(jnp.float32))
        return hits

    def analyse(block):
        hits = gathered(block)
        zero = jnp.zeros(shape, jnp.float32)
        found, named, column = [zero] * share, zero, zero
        for k in range(names.shape[0]):
            here = (source == panels[k : k + 1, :]).astype(jnp.float32)
            named += here
            column += here * inside[k : k + 1, :].astype(jnp.float32)
            for u in range(share):
                found[u] += here * hits[u][k : k + 1, :]
        found = [jnp.where(other, product(value, groups), 0.0) > 0.5 for value in found]
        named = jnp.maximum(product(named, groups), 1.0)
        column = jnp.floor(product(column, groups) / named + 0.5)
        both = jnp.logical_and(found[0], found[1])
        away = jnp.logical_and(both, jnp.logical_not(same_level)).astype(jnp.float32)
        return found, column, both, away, product(away, spread)

    def fits():
        misfit = jnp.zeros(shape, jnp.float32)
        for block in range(4):
            found, _, both, away, riding = analyse(block)
            need = jnp.logical_or(found[0], found[1])
            crowded = jnp.logical_or(
                riding > 1.5, jnp.logical_and(riding > 0.5, jnp.logical_or(need, both))
            )
            misfit += jnp.where(
                jnp.logical_and(same_level, jnp.logical_or(crowded, both)), 1.0, 0.0
            )
            arriving = product(same_level.astype(jnp.float32), away)
            misfit += jnp.where(jnp.logical_and(valid, arriving > 1.5), 1.0, 0.0)
        total = jnp.sum(jnp.sum(misfit, axis=0, keepdims=True), axis=1, keepdims=True)
        line = jnp.broadcast_to((total > 0.5).astype(jnp.int32), (1, LANES))
        plan_ref[pl.ds(MISFIT, 1), :] = line

    if whole:
        fits()
    if steps is False:
        return

    found, column, both, away, riding = analyse(row)
    need = jnp.logical_or(found[0], found[1])
    direct = column + jnp.where(found[0], 0.0, float(TILE_BIT)) + SENT_BIT
    ride = product(away * column, spread) + TILE_BIT + SENT_BIT
    taken = jnp.logical_and(same_level, riding > 0.5)
    code = jnp.where(need, direct, jnp.where(taken, ride, 0.0))
    mine = (lax.broadcasted_iota(jnp.int32, (8, LANES), 1) == place).astype(jnp.float32)
    level_row = (
        lax.div(lax.broadcasted_iota(jnp.int32, (8, LANES), 1), depth) == lax.div(place, depth)
    ).astype(jnp.float32)
    first = lax.dot_general(
        mine.astype(jnp.bfloat16), found[0].astype(jnp.float32).astype(jnp.bfloat16),
        (((1,), (1,)), ((), ())), preferred_element_type=jnp.float32,
    )
    hop = product(level_row, away * (down + 1).astype(jnp.float32))
    grid_ref[0] = code
    grid_ref[1] = jnp.where(both, column + (TILE_BIT + SENT_BIT), 0.0)
    plan_ref[pl.ds(SEND, 1), :] = grid_ref[0, pl.ds(place, 1), :].astype(jnp.int32)
    plan_ref[pl.ds(FIRST, 1), :] = first[:1].astype(jnp.int32)
    plan_ref[pl.ds(HOP, 1), :] = hop[:1].astype(jnp.int32)
    plan_ref[pl.ds(SECOND, 1), :] = grid_ref[1, pl.ds(place, 1), :].astype(jnp.int32)


def plans_kernel(parts, order_ref, first_ref, second_ref, *rest):
    *plan_refs, grid_ref, line_ref = rest
    for (permuted, steps, whole), plan_ref in zip(parts, plan_refs):
        in_ref = second_ref if permuted else first_ref
        plan_kernel(
            permuted, steps, whole, order_ref, in_ref, second_ref, plan_ref, grid_ref, line_ref
        )


def plans(parts, order_line, first_rows, second_rows):
    work = sum((1 if steps else 0) + (4 if whole else 0) for _, steps, whole in parts)
    return pl.pallas_call(
        functools.partial(plans_kernel, parts),
        out_shape=(jax.ShapeDtypeStruct((8, LANES), jnp.int32),) * len(parts),
        in_specs=[VMEM, VMEM, VMEM],
        out_specs=(VMEM,) * len(parts),
        scratch_shapes=[
            pltpu.VMEM((2, LANES, LANES), jnp.float32),
            pltpu.VMEM((8, LANES), jnp.int32),
        ],
        cost_estimate=pl.CostEstimate(
            flops=work << 23, bytes_accessed=1 << 14, transcendentals=0
        ),
    )(order_line, first_rows, second_rows)


def column_kernel(x_ref, part_ref):
    part_ref[...] = jnp.sum(x_ref[...], axis=(1, 2))


def column_partial(x):
    return pl.pallas_call(
        column_kernel,
        out_shape=jax.ShapeDtypeStruct((x.shape[0], x.shape[-1]), jnp.float32),
        in_specs=[VMEM],
        out_specs=VMEM,
        cost_estimate=pl.CostEstimate(flops=x.size, bytes_accessed=4 * x.size, transcendentals=0),
    )(x)


def send_kernel(line, plan_ref, x_ref, *rest):
    *sums, send_ref, normal, sems = rest
    panels = send_ref.shape[0]
    total = sums[0][...]
    for part in sums[1:]:
        total += part[...]
    normal[...] = x_ref[...] / total[:, None, None, :]

    def each(act):
        @pl.loop(0, panels)
        def _(slot):
            code = plan_ref[line, slot]

            @pl.when(code >= SENT_BIT)
            def _():
                tile = normal.at[code & 3, (code // TILE_BIT) & 1]
                act(pltpu.make_async_copy(tile, send_ref.at[slot], sems.at[slot]))

    each(lambda piece: piece.start())
    each(lambda piece: piece.wait())


def prepare(line, steps, x, sums, panels):
    tile = x.shape[-1]
    return pl.pallas_call(
        functools.partial(send_kernel, line),
        out_shape=jax.ShapeDtypeStruct((panels, tile, tile), jnp.float32),
        in_specs=[SMEM, VMEM] + [VMEM] * len(sums),
        out_specs=ANY,
        scratch_shapes=[
            pltpu.VMEM(x.shape, jnp.float32),
            pltpu.SemaphoreType.DMA((panels,)),
        ],
        cost_estimate=pl.CostEstimate(flops=x.size, bytes_accessed=3 << 20, transcendentals=0),
    )(steps, x, *sums)


def hop_kernel(plan_ref, got_ref, *rest):
    *outs, sems = rest
    place = lax.axis_index("pcol")
    depth = got_ref.shape[0] // 4
    pieces = []
    for step, out in enumerate(outs):
        target = lax.rem(place + (step + 1) * depth, 4 * depth)
        slot = jnp.maximum(plan_ref[HOP, target] - 1, 0)
        pieces.append(pltpu.make_async_copy(got_ref.at[slot], out, sems.at[step]))
    for piece in pieces:
        piece.start()
    for piece in pieces:
        piece.wait()


def hop_tiles(steps, got):
    tile = jax.ShapeDtypeStruct(got.shape[1:], jnp.float32)
    return pl.pallas_call(
        hop_kernel,
        out_shape=(tile,) * 3,
        in_specs=[SMEM, ANY],
        out_specs=(VMEM,) * 3,
        scratch_shapes=[pltpu.SemaphoreType.DMA((3,))],
        cost_estimate=pl.CostEstimate(flops=0, bytes_accessed=6 << 16, transcendentals=0),
    )(steps, got)


def split(value):
    high = value.astype(jnp.bfloat16)
    low = (value - high.astype(jnp.float32)).astype(jnp.bfloat16)
    return high, low


def dot_exactly(left, right):
    left_high, left_low = split(left)
    right_high, right_low = split(right)
    dot = functools.partial(jnp.dot, preferred_element_type=jnp.float32)
    return (dot(left_low, right_high) + dot(left_high, right_low)) + dot(left_high, right_high)


FIRSTS, SECONDS, LIST = 2, 64, 128


def matched(in_ref, out_pat_ref, row, share, own_column, column, t):
    wanted = out_pat_ref[row * share + t, own_column]
    hit = wanted < 0
    at = 0
    for u in range(share):
        same = in_ref[row * share + u, column] == wanted
        hit = jnp.logical_or(hit, same)
        at = jnp.where(same, u, at)
    return hit, at


def list_kernel(permuted, cols, share, order_ref, plan_ref, in_ref, out_pat_ref, list_ref):
    row = lax.axis_index("prow")
    panel = order_ref[lax.axis_index("pcol")]
    names = in_ref.shape[0]

    def remote(place_of, counts):
        own_column = panel * cols + place_of // names
        column = in_ref[lax.rem(place_of, names), own_column]
        source = column // cols
        origin = order_ref[source] if permuted else source
        firsts, seconds = counts
        for t in range(share):
            hit, at = matched(in_ref, out_pat_ref, row, share, own_column, column, t)
            hit = jnp.logical_and(hit, source != panel)
            extra = jnp.logical_and(hit, jnp.logical_and(at == 1, plan_ref[FIRST, origin] > 0))
            simple = jnp.logical_and(hit, jnp.logical_not(extra))
            entry = (place_of * share + t) * 32 + origin

            @pl.when(simple)
            def _():
                list_ref[FIRSTS + firsts] = entry

            @pl.when(extra)
            def _():
                list_ref[SECONDS + seconds] = entry

            firsts = firsts + simple.astype(jnp.int32)
            seconds = seconds + extra.astype(jnp.int32)
        return firsts, seconds

    firsts, seconds = lax.fori_loop(0, cols * names, remote, (jnp.int32(0), jnp.int32(0)))
    list_ref[0] = firsts
    list_ref[1] = seconds


def tile_list(permuted, cols, share, order, steps, in_pattern, out_pattern):
    return pl.pallas_call(
        functools.partial(list_kernel, permuted, cols, share),
        out_shape=jax.ShapeDtypeStruct((LIST,), jnp.int32),
        in_specs=[SMEM] * 4,
        out_specs=SMEM,
        cost_estimate=pl.CostEstimate(flops=1 << 28, bytes_accessed=1 << 14, transcendentals=0),
    )(order, steps, in_pattern, out_pattern)


def own_kernel(
    order_ref, in_ref, out_pat_ref,
    own_ref, ahead_ref, behind_ref, far_low_ref, far_high_ref,
    base_ref, totals_ref, right_ref,
):
    cols, share, tile, _ = own_ref.shape
    row = lax.axis_index("prow")
    rows = right_ref.shape[1] // share
    panel = order_ref[lax.axis_index("pcol")]
    home = panel // (order_ref.shape[0] // rows)
    half = cols // 2

    for rel in range(4):
        first = lax.rem(row + rel, rows) * share
        for j in range(cols):
            far = far_low_ref.at[j] if j < half else far_high_ref.at[j - half]
            piece = (own_ref.at[j], ahead_ref.at[j], far, behind_ref.at[j])[rel]
            right_ref[j, pl.ds(first, share)] = piece[...]
    for j in range(cols):
        whole = right_ref[j].reshape(rows * share * tile, tile)
        totals_ref[pl.ds(j, 1), :] = jnp.sum(whole, axis=0, keepdims=True)

    @pl.loop(0, cols)
    def _(j):
        base_ref[j] = jnp.zeros((share, tile, tile), jnp.float32)
        for s in range(share):
            k = home * share + s
            own_column = panel * cols + j
            column = in_ref[k, own_column]
            local = lax.rem(column, cols)
            for t in range(share):
                hit, at = matched(in_ref, out_pat_ref, row, share, own_column, column, t)

                @pl.when(jnp.logical_and(hit, column // cols == panel))
                def _():
                    left = own_ref[local, at] / totals_ref[pl.ds(local, 1), :]
                    base_ref[j, t] += dot_exactly(left, right_ref[j, k])


def own_products(order, in_pattern, out_pattern, own, gathered):
    cols, share, tile, _ = own.shape
    return pl.pallas_call(
        own_kernel,
        out_shape=(
            jax.ShapeDtypeStruct(own.shape, jnp.float32),
            jax.ShapeDtypeStruct((cols, tile), jnp.float32),
            jax.ShapeDtypeStruct((cols, 4 * share, tile, tile), jnp.float32),
        ),
        in_specs=[SMEM] * 3 + [VMEM] * 5,
        out_specs=(VMEM, VMEM, VMEM),
        cost_estimate=pl.CostEstimate(flops=1 << 26, bytes_accessed=5 << 20, transcendentals=0),
    )(order, in_pattern, out_pattern, own, *gathered)


def shifts(x, panels):
    up = [(i, i + 1) for i in range(panels - 1)]
    from_below = lax.ppermute(x, "pcol", up)
    from_above = lax.ppermute(x, "pcol", [(j, i) for i, j in up])
    return from_below, from_above


def add_listed(list_ref, number, first, right_ref, acc_ref, fetch, lefts, rights, sems):
    share = acc_ref.shape[1]
    names = right_ref.shape[1]
    count = list_ref[number]

    def where(i):
        entry = list_ref[first + i]
        spot = entry // 32
        column_slot = spot // share
        return (
            column_slot // names, lax.rem(column_slot, names), lax.rem(spot, share),
            lax.rem(entry, 32),
        )

    def right_copy(i, j, k):
        return pltpu.make_async_copy(right_ref.at[j, k], rights.at[i], sems.at[1, i])

    @pl.loop(0, count)
    def _(i):
        j, k, _, origin = where(i)
        right_copy(i, j, k).start()
        fetch(i, origin)

    @pl.loop(0, count)
    def _(i):
        j, k, t, _ = where(i)
        right_copy(i, j, k).wait()
        pltpu.make_async_copy(right_ref.at[j, k], lefts.at[i], sems.at[0, i]).wait()
        acc_ref[j, t] += dot_exactly(lefts[i], rights[i])


def main_kernel(list_ref, base_ref, right_ref, got_ref, acc_ref, lefts, rights, sems):
    acc_ref[...] = base_ref[...]

    def fetch(i, origin):
        pltpu.make_async_copy(got_ref.at[origin], lefts.at[i], sems.at[0, i]).start()

    add_listed(list_ref, 0, FIRSTS, right_ref, acc_ref, fetch, lefts, rights, sems)


def last_kernel(depth, list_ref, acc_in_ref, totals_ref, right_ref, *rest):
    *extra_refs, sq_ref, part_ref, lefts, rights, sems = rest
    cols, share, tile, _ = acc_in_ref.shape
    place = lax.axis_index("pcol")
    sq_ref[...] = acc_in_ref[...]

    def fetch(i, origin):
        if len(extra_refs) == 1:
            pltpu.make_async_copy(extra_refs[0].at[origin], lefts.at[i], sems.at[0, i]).start()
            return
        step = lax.rem(place // depth - origin // depth + 4, 4)
        for distance, ref in enumerate(extra_refs):

            @pl.when(step == distance + 1)
            def _():
                pltpu.make_async_copy(ref, lefts.at[i], sems.at[0, i]).start()

    add_listed(list_ref, 1, SECONDS, right_ref, sq_ref, fetch, lefts, rights, sems)
    for j in range(cols):
        value = sq_ref[j].reshape(share * tile, tile) / totals_ref[pl.ds(j, 1), :]
        square = value * value
        sq_ref[j] = square.reshape(share, tile, tile)
        part_ref[pl.ds(j, 1), :] = jnp.sum(square, axis=0, keepdims=True)


def list_scratch(right):
    _, _, tile, _ = right.shape
    most = SECONDS - FIRSTS - 2
    return [
        pltpu.VMEM((most, tile, tile), jnp.float32),
        pltpu.VMEM((most, tile, tile), jnp.float32),
        pltpu.SemaphoreType.DMA((2, most)),
    ]


def main_products(tiles, base, right, got):
    return pl.pallas_call(
        main_kernel,
        out_shape=jax.ShapeDtypeStruct(base.shape, jnp.float32),
        in_specs=[SMEM, VMEM, ANY, ANY],
        out_specs=VMEM,
        scratch_shapes=list_scratch(right),
        cost_estimate=pl.CostEstimate(flops=1 << 30, bytes_accessed=3 << 20, transcendentals=0),
    )(tiles, base, right, got)


def last_products(depth, tiles, acc, totals, right, extra):
    cols, _, tile, _ = acc.shape
    return pl.pallas_call(
        functools.partial(last_kernel, depth),
        out_shape=(
            jax.ShapeDtypeStruct(acc.shape, jnp.float32),
            jax.ShapeDtypeStruct((cols, tile), jnp.float32),
        ),
        in_specs=[SMEM, VMEM, VMEM, ANY] + [ANY] * len(extra),
        out_specs=(VMEM, VMEM),
        scratch_shapes=list_scratch(right),
        cost_estimate=pl.CostEstimate(flops=1 << 24, bytes_accessed=2 << 20, transcendentals=0),
    )(tiles, acc, totals, right, *extra)


def divide_kernel(x_ref, *rest):
    *sums, out_ref = rest
    total = sums[0][...]
    for part in sums[1:]:
        total += part[...]
    out_ref[...] = x_ref[...] / total[:, None, None, :]


def divided(x, sums):
    return pl.pallas_call(
        divide_kernel,
        out_shape=jax.ShapeDtypeStruct(x.shape, jnp.float32),
        in_specs=[VMEM] * (1 + len(sums)),
        out_specs=VMEM,
        cost_estimate=pl.CostEstimate(flops=x.size, bytes_accessed=1 << 20, transcendentals=0),
    )(x, *sums)


def gather_rows(own, size):
    half = own.shape[0] // 2
    behind = lax.ppermute(own, "prow", ring(size, 1))
    ahead = lax.ppermute(own, "prow", ring(size, -1))
    far_low = lax.ppermute(behind[:half], "prow", ring(size, 1))
    far_high = lax.ppermute(ahead[half:], "prow", ring(size, -1))
    return ahead, behind, far_low, far_high


def expand(permuted, order, steps, misfit, in_pattern, out_pattern, x, sums, own, rows):
    cols, share = x.shape[:2]
    panels = order.shape[0]
    depth = panels // 4
    send = prepare(SEND, steps, x, sums, panels)
    got = lax.all_to_all(send, "pcol", 0, 0, tiled=True)
    tiles = tile_list(permuted, cols, share, order, steps, in_pattern, out_pattern)
    gathered = gather_rows(own, rows)
    base, totals, right = own_products(order, in_pattern, out_pattern, own, gathered)

    def by_level(_):
        hops = hop_tiles(steps, got)
        extra = tuple(
            lax.ppermute(tile, "pcol", ring(panels, (step + 1) * depth))
            for step, tile in enumerate(hops)
        )
        acc = main_products(tiles, base, right, got)
        return last_products(depth, tiles, acc, totals, right, extra)

    def by_second(_):
        more = prepare(SECOND, steps, x, sums, panels)
        extra = (lax.all_to_all(more, "pcol", 0, 0, tiled=True),)
        acc = main_products(tiles, base, right, got)
        return last_products(depth, tiles, acc, totals, right, extra)

    return lax.cond(misfit > 0, by_second, by_level, 0)


def local(match_tiles, pattern, kept, panel_order):
    rows = lax.axis_size("prow")
    order = panel_order
    pattern_rows = pattern.T
    kept_rows = kept.T
    tables = (order[None], pattern_rows, kept_rows)
    (first_plan,) = plans(((False, True, False),), *tables)
    from_below, from_above = shifts(match_tiles, order.shape[0])
    sums = row_sums(column_partial(match_tiles), rows)
    place = lax.axis_index("pcol")
    step = order[place] - place
    sums, step = lax.optimization_barrier((sums, step))
    own = jnp.where(step == 0, match_tiles, jnp.where(step < 0, from_below, from_above))
    check, second_plan = plans(((False, False, True), (True, True, True)), *tables)
    square, part = expand(
        False, order, first_plan, check[MISFIT, 0], pattern_rows, kept_rows,
        match_tiles, sums, own, rows,
    )
    sums = row_sums(part, rows)
    square, part = expand(
        True, order, second_plan, second_plan[MISFIT, 0], kept_rows, kept_rows,
        square, sums, square, rows,
    )
    return divided(square, row_sums(part, rows))


def solution(mesh):
    in_specs = (P("pcol", "prow", None, None), P(), P(), P())
    out_specs = P("pcol", "prow", None, None)
    return jax.shard_map(local, mesh=mesh, in_specs=in_specs, out_specs=out_specs, check_vma=False)
```
